8 devices in a mesh: dp: 2 (over z, y), tp: 4 (over x, core).
Axes of the slice: x: 2, y: 2, z: 1, core: 2. Of those that a mesh axis runs over, the one named last changes fastest.
Arguments:
- hidden: bfloat16 [48, 2560], P('dp'), parts along dimension 0
- positions: int32 [48], P('dp'), parts along dimension 0
- k_local: bfloat16 [48, 1024, 4, 256], P('dp', None, 'tp'), parts along dimension 0
- v_local: bfloat16 [48, 1024, 4, 256], P('dp', None, 'tp'), parts along dimension 0
- k_global: bfloat16 [48, 2048, 4, 256], P('dp', None, 'tp'), parts along dimension 0
- v_global: bfloat16 [48, 2048, 4, 256], P('dp', None, 'tp'), parts along dimension 0
- w_query: bfloat16 [2, 2560, 2048], P(None, None, 'tp')
- w_key: bfloat16 [2, 2560, 1024], P(None, None, 'tp')
- w_value: bfloat16 [2, 2560, 1024], P(None, None, 'tp')
- w_out: bfloat16 [2, 2048, 2560], P(None, 'tp')
- w_gate: bfloat16 [2, 2560, 10240], P(None, None, 'tp')
- w_up: bfloat16 [2, 2560, 10240], P(None, None, 'tp')
- w_down: bfloat16 [2, 10240, 2560], P(None, 'tp')
- norm_scale: float32 [2, 4, 2560], replicated
Outputs:
- output 1: bfloat16 [48, 2560], P('dp'), parts along dimension 0
- output 2: bfloat16 [48, 1024, 4, 256], P('dp', None, 'tp'), parts along dimension 0
- output 3: bfloat16 [48, 1024, 4, 256], P('dp', None, 'tp'), parts along dimension 0
- output 4: bfloat16 [48, 2048, 4, 256], P('dp', None, 'tp'), parts along dimension 0
- output 5: bfloat16 [48, 2048, 4, 256], P('dp', None, 'tp'), parts along dimension 0
There are 2 independent parts. The reference program is written for one: setup_inputs(seed, part) draws one part's arguments, and reference() takes and returns one part's arrays. A program takes and returns all parts, laid end to end along the dimension named above; an argument that names none is the same for every part.
All inputs are finite; a program needn't handle non-finite values.
Results may differ from the reference program's by a relative error of at most 0.02.
Values are sent between devices in bfloat16 or wider.
A program may use at most 1 GiB of HBM per device.

```python
import jax
import jax.numpy as jnp
from jax import lax

D = 2560
HEADS = 8
KV_HEADS = 4
HEAD = 256
FF = 10240
WINDOW = 1024
BATCH = 24
CTX = 2048

SOFT_CAP = 50.0
NORM_EPS = 1e-6
ROPE_BASE = 10000.0
NEG_FILL = -1e30


def draw_positions(pos_key):
    draw_key, row_key = jax.random.split(pos_key)
    drawn_pos = jax.random.randint(draw_key, (BATCH,), WINDOW, CTX, dtype=jnp.int32)
    top_row = jax.random.randint(row_key, (), 0, BATCH, dtype=jnp.int32)
    row_ids = jnp.arange(BATCH, dtype=jnp.int32)
    return jnp.where(row_ids == top_row, CTX - 1, drawn_pos).astype(jnp.int32)


def normal_bf16(rand_key, arr_shape, std_scale):
    return (jax.random.normal(rand_key, arr_shape, jnp.float32) * std_scale).astype(jnp.bfloat16)


def setup_inputs(seed: int = 0, part: int = 0) -> dict:
    part_key = jax.random.fold_in(jax.random.key(seed), part)
    row_keys = jax.random.split(part_key, 6)
    weight_keys = jax.random.split(jax.random.key(seed + 1), 8)
    value_gain = jnp.sqrt(jnp.array([WINDOW, CTX], dtype=jnp.float32)).reshape(2, 1, 1)
    return {
        'hidden': normal_bf16(row_keys[0], (BATCH, D), 1.0),
        'positions': draw_positions(row_keys[1]),
        'k_local': normal_bf16(row_keys[2], (BATCH, WINDOW, KV_HEADS, HEAD), 1.0),
        'v_local': normal_bf16(row_keys[3], (BATCH, WINDOW, KV_HEADS, HEAD), 1.0),
        'k_global': normal_bf16(row_keys[4], (BATCH, CTX, KV_HEADS, HEAD), 1.0),
        'v_global': normal_bf16(row_keys[5], (BATCH, CTX, KV_HEADS, HEAD), 1.0),
        'w_query': normal_bf16(weight_keys[0], (2, D, HEADS * HEAD), D ** -0.5),
        'w_key': normal_bf16(weight_keys[1], (2, D, KV_HEADS * HEAD), D ** -0.5),
        'w_value': normal_bf16(weight_keys[2], (2, D, KV_HEADS * HEAD), value_gain * D ** -0.5),
        'w_out': normal_bf16(weight_keys[3], (2, HEADS * HEAD, D), (HEADS * HEAD) ** -0.5),
        'w_gate': normal_bf16(weight_keys[4], (2, D, FF), D ** -0.5),
        'w_up': normal_bf16(weight_keys[5], (2, D, FF), D ** -0.5),
        'w_down': normal_bf16(weight_keys[6], (2, FF, D), FF ** -0.5),
        'norm_scale': jax.random.normal(weight_keys[7], (2, 4, D), jnp.float32) * 0.4,
    }


def rms_norm(values, gain_row):
    values_f32 = values.astype(jnp.float32)
    inv_rms = lax.rsqrt(jnp.mean(values_f32 * values_f32, axis=-1, keepdims=True) + NORM_EPS)
    return (values_f32 * inv_rms * (1.0 + gain_row)).astype(jnp.bfloat16)


def rotary(projected, positions):
    half_dim = HEAD // 2
    inv_freq = ROPE_BASE ** (-2.0 * jnp.arange(half_dim, dtype=jnp.float32) / HEAD)
    angles = positions.astype(jnp.float32)[:, None, None] * inv_freq
    cos_part = jnp.cos(angles)
    sin_part = jnp.sin(angles)
    first_half = projected[..., :half_dim]
    second_half = projected[..., half_dim:]
    return jnp.concatenate([first_half * cos_part - second_half * sin_part, second_half * cos_part + first_half * sin_part], axis=-1)


def attend_row(row_args):
    queries, key_rows, value_rows, key_valid = row_args
    logits = jnp.einsum('grd,ngd->grn', queries.astype(jnp.float32), key_rows.astype(jnp.float32)) * HEAD ** -0.5
    logits = SOFT_CAP * jnp.tanh(logits / SOFT_CAP)
    logits = jnp.where(key_valid[None, None, :], logits, NEG_FILL)
    attn_probs = jax.nn.softmax(logits, axis=-1).astype(jnp.bfloat16)
    mixed_heads = jnp.einsum('grn,ngd->grd', attn_probs.astype(jnp.float32), value_rows.astype(jnp.float32))
    return mixed_heads.astype(jnp.bfloat16)


def add_normed(hidden, branch_sum, gain_row):
    return (hidden.astype(jnp.float32) + rms_norm(branch_sum, gain_row).astype(jnp.float32)).astype(jnp.bfloat16)


def decoder_layer(hidden, positions, k_cache, v_cache, slot_ids, key_valid, layer_weights, gains):
    w_query, w_key, w_value, w_out, w_gate, w_up, w_down = layer_weights
    normed = rms_norm(hidden, gains[0])
    queries = jnp.dot(normed, w_query, preferred_element_type=jnp.float32).reshape(BATCH, HEADS, HEAD)
    key_new = jnp.dot(normed, w_key, preferred_element_type=jnp.float32).reshape(BATCH, KV_HEADS, HEAD)
    value_new = jnp.dot(normed, w_value, preferred_element_type=jnp.float32).astype(jnp.bfloat16).reshape(BATCH, KV_HEADS, HEAD)
    queries = rotary(queries, positions).astype(jnp.bfloat16)
    key_new = rotary(key_new, positions).astype(jnp.bfloat16)
    slot_hit = (jnp.arange(k_cache.shape[1])[None, :] == slot_ids[:, None])[:, :, None, None]
    k_cache = jnp.where(slot_hit, key_new[:, None], k_cache)
    v_cache = jnp.where(slot_hit, value_new[:, None], v_cache)
    grouped = queries.reshape(BATCH, KV_HEADS, HEADS // KV_HEADS, HEAD)
    mixed_heads = lax.map(attend_row, (grouped, k_cache, v_cache, key_valid))
    attn_sum = jnp.dot(mixed_heads.reshape(BATCH, HEADS * HEAD), w_out, preferred_element_type=jnp.float32)
    hidden = add_normed(hidden, attn_sum, gains[1])
    normed = rms_norm(hidden, gains[2])
    gate_proj = jnp.dot(normed, w_gate, preferred_element_type=jnp.float32)
    up_proj = jnp.dot(normed, w_up, preferred_element_type=jnp.float32)
    hidden_act = (jax.nn.gelu(gate_proj, approximate=True) * up_proj).astype(jnp.bfloat16)
    down_sum = jnp.dot(hidden_act, w_down, preferred_element_type=jnp.float32)
    hidden = add_normed(hidden, down_sum, gains[3])
    return hidden, k_cache, v_cache


def reference(hidden, positions, k_local, v_local, k_global, v_global, w_query, w_key, w_value, w_out, w_gate, w_up, w_down, norm_scale):
    stacks = (w_query, w_key, w_value, w_out, w_gate, w_up, w_down)
    local_valid = jnp.full((BATCH, WINDOW), True)
    global_valid = jnp.arange(CTX)[None, :] <= positions[:, None]
    hidden, k_local, v_local = decoder_layer(hidden, positions, k_local, v_local, positions % WINDOW, local_valid, tuple(stacked[0] for stacked in stacks), norm_scale[0])
    hidden, k_global, v_global = decoder_layer(hidden, positions, k_global, v_global, positions, global_valid, tuple(stacked[1] for stacked in stacks), norm_scale[1])
    return (hidden, k_local, v_local, k_global, v_global)
```

```python
import functools

import jax
import jax.numpy as jnp
import numpy as np
from jax import lax
from jax.experimental import pallas as pl
from jax.experimental.pallas import tpu as pltpu
from jax.sharding import PartitionSpec as P

SOFT_CAP = 50.0
NORM_EPS = 1e-6
ROPE_BASE = 10000.0
ROWS = 24
D = 2560
HEAD = 256
HALF = 128
GROUP = 4
SLOTS = 4
CHUNK = 512
F32 = jnp.float32
BF16 = jnp.bfloat16


def normed(values, gain_row):
    inv_rms = lax.rsqrt(jnp.mean(values * values, axis=-1, keepdims=True) + NORM_EPS)
    return (values * inv_rms * (1.0 + gain_row)).astype(BF16)


def attn_kernel(layer, masked, pos_hbm, x_hbm, gain_hbm, freq_hbm, wq_hbm, wk_hbm, wv_hbm, wo_hbm, kc_hbm, vc_hbm,
                ko_hbm, vo_hbm, o_ref,
                pos, x, gain, freq, wq, wk, wv, wo, kbuf, vbuf, qa, qb, ma, mb, knew, vnew,
                small_sem, w_sem, kr_sem, vr_sem, kw_sem, vw_sem):
    n = kc_hbm.shape[1]
    groups = ROWS // GROUP

    def rows_of(ref, g):
        return ref.at[pl.ds(g * GROUP, GROUP)]

    def read(g, slot):
        pltpu.make_async_copy(rows_of(kc_hbm, g), kbuf.at[slot], kr_sem.at[slot]).start()
        pltpu.make_async_copy(rows_of(vc_hbm, g), vbuf.at[slot], vr_sem.at[slot]).start()

    small = [pltpu.make_async_copy(s, d, small_sem.at[i]) for i, (s, d) in enumerate(
        ((x_hbm, x), (gain_hbm.at[layer], gain), (pos_hbm, pos), (freq_hbm, freq)))]
    weights = [pltpu.make_async_copy(s.at[layer], d, w_sem.at[i]) for i, (s, d) in enumerate(
        ((wq_hbm, wq), (wk_hbm, wk), (wv_hbm, wv), (wo_hbm, wo)))]
    for copy in small:
        copy.start()
    for copy in weights[:3]:
        copy.start()
    for g in range(SLOTS):
        read(g, g)
    weights[3].start()

    for copy in small:
        copy.wait()
    a = normed(x[...].astype(F32), gain[0:1, :])
    row_ids = lax.broadcasted_iota(jnp.int32, (ROWS, HALF), 0)
    pos_rows = jnp.zeros((ROWS, HALF), jnp.int32)
    for b in range(ROWS):
        pos_rows = jnp.where(row_ids == b, pos[b], pos_rows)
    angles = pos_rows.astype(F32) * freq[...]
    cos_part = jnp.cos(angles)
    sin_part = jnp.sin(angles)

    def rotate(t):
        first, second = t[:, :HALF], t[:, HALF:]
        return first * cos_part - second * sin_part, second * cos_part + first * sin_part

    weights[0].wait()
    q = jnp.dot(a, wq[...], preferred_element_type=F32)
    for h in range(2):
        first, second = rotate(q[:, h * HEAD:(h + 1) * HEAD])
        qa[pl.ds(h, ROWS, stride=2), :] = first
        qb[pl.ds(h, ROWS, stride=2), :] = second
    weights[1].wait()
    first, second = rotate(jnp.dot(a, wk[...], preferred_element_type=F32))
    knew[:, :HALF] = first
    knew[:, HALF:] = second
    weights[2].wait()
    vnew[...] = jnp.dot(a, wv[...], preferred_element_type=F32)

    def patch(buf, slot, j, row, b, new):
        base = pl.multiple_of((row // 16) * 16, 16)
        tile = buf[slot, j, pl.ds(base, 16), :].astype(F32)
        hit = lax.broadcasted_iota(jnp.int32, (16, HEAD), 0) == row - base
        fresh = jnp.broadcast_to(new[pl.ds(b, 1), :], (16, HEAD))
        buf[slot, j, pl.ds(base, 16), :] = jnp.where(hit, fresh, tile).astype(BF16)

    def write_copies(g, slot):
        return (pltpu.make_async_copy(kbuf.at[slot], rows_of(ko_hbm, g), kw_sem.at[slot]),
                pltpu.make_async_copy(vbuf.at[slot], rows_of(vo_hbm, g), vw_sem.at[slot]))

    def step(g, carry):
        slot = lax.rem(g, SLOTS)
        pltpu.make_async_copy(rows_of(kc_hbm, g), kbuf.at[slot], kr_sem.at[slot]).wait()
        for j in range(GROUP):
            b = g * GROUP + j
            patch(kbuf, slot, j, lax.rem(pos[b], n), b, knew)
        q8 = jnp.concatenate([qa[pl.ds(pl.multiple_of(g * 8, 8), 8), :], qb[pl.ds(pl.multiple_of(g * 8, 8), 8), :]], axis=1).astype(BF16)
        owner = lax.broadcasted_iota(jnp.int32, (8, n), 0) // 2
        s = None
        for j in range(GROUP):
            part = lax.dot_general(q8, kbuf[slot, j], (((1,), (1,)), ((), ())), preferred_element_type=F32)
            s = part if s is None else jnp.where(owner == j, part, s)
        e = jnp.exp(SOFT_CAP * jnp.tanh(s * (HEAD ** -0.5 / SOFT_CAP)))
        if masked:
            limit_rows = lax.broadcasted_iota(jnp.int32, (8, 1), 0) // 2
            limit = jnp.zeros((8, 1), jnp.int32)
            for j in range(GROUP):
                limit = jnp.where(limit_rows == j, pos[g * GROUP + j], limit)
            e = jnp.where(lax.broadcasted_iota(jnp.int32, (8, n), 1) <= limit, e, 0.0)
        p = (e / jnp.sum(e, axis=-1, keepdims=True)).astype(BF16)
        pltpu.make_async_copy(rows_of(vc_hbm, g), vbuf.at[slot], vr_sem.at[slot]).wait()
        for j in range(GROUP):
            b = g * GROUP + j
            patch(vbuf, slot, j, lax.rem(pos[b], n), b, vnew)
        owner = lax.broadcasted_iota(jnp.int32, (8, HEAD), 0) // 2
        m = None
        for j in range(GROUP):
            part = jnp.dot(p, vbuf[slot, j], preferred_element_type=F32)
            m = part if m is None else jnp.where(owner == j, part, m)
        ma[pl.ds(pl.multiple_of(g * 8, 8), 8), :] = m[:, :HALF]
        mb[pl.ds(pl.multiple_of(g * 8, 8), 8), :] = m[:, HALF:]
        for copy in write_copies(g, slot):
            copy.start()

        @pl.when(g >= 1)
        def _():
            before = lax.rem(g + SLOTS - 1, SLOTS)
            for copy in write_copies(g - 1, before):
                copy.wait()

            @pl.when(g + SLOTS - 1 < groups)
            def _():
                read(g + SLOTS - 1, before)
        return carry

    lax.fori_loop(0, groups, step, 0)

    mixed = jnp.concatenate([ref[pl.ds(h, ROWS, stride=2), :] for h in range(2) for ref in (ma, mb)], axis=1).astype(BF16)
    weights[3].wait()
    for c in range(D // CHUNK):
        o_ref[c] = jnp.dot(mixed, wo[:, c * CHUNK:(c + 1) * CHUNK], preferred_element_type=F32).astype(BF16)
    for copy in write_copies(groups - 1, (groups - 1) % SLOTS):
        copy.wait()


def mlp_kernel(layer, x_hbm, o_hbm, gain_hbm, wg_hbm, wu_hbm, wd_hbm, out_ref,
               x, gain, wg, wu, wd, h, osend, ohalf, orecv1, orecv2, fsend, fhalf, frecv1, frecv2, total,
               small_sem, g_sem, u_sem, d_sem, os1, or1, os2, or2, fs1, fr1, fs2, fr2):
    chunks = D // CHUNK
    me = lax.axis_index("tp")
    chip, core = me // 2, lax.rem(me, 2)
    partner = chip * 2 + (1 - core)
    across = (1 - chip) * 2 + core

    small = [pltpu.make_async_copy(s, d, small_sem.at[i]) for i, (s, d) in enumerate(
        ((o_hbm, osend), (x_hbm, x), (gain_hbm.at[layer], gain)))]
    for copy in small:
        copy.start()
    cols = [pl.ds(c * CHUNK, CHUNK) for c in range(chunks)]
    gates = [pltpu.make_async_copy(wg_hbm.at[layer, :, cols[c]], wg.at[c], g_sem.at[c]) for c in range(chunks)]
    ups = [pltpu.make_async_copy(wu_hbm.at[layer, :, cols[c]], wu.at[c], u_sem.at[c]) for c in range(chunks)]
    downs = [pltpu.make_async_copy(wd_hbm.at[layer, :, cols[c]], wd.at[c], d_sem.at[c]) for c in range(chunks)]
    for c in range(chunks):
        gates[c].start()
        ups[c].start()
    for c in range(chunks):
        downs[c].start()

    barrier = pltpu.get_barrier_semaphore()
    for peer in (partner, across):
        pl.semaphore_signal(barrier, inc=1, device_id={"tp": peer}, device_id_type=pl.DeviceIdType.MESH)
    pl.semaphore_wait(barrier, 2)

    def remote(src, dst, send, recv, c, peer):
        return pltpu.make_async_remote_copy(src_ref=src.at[c], dst_ref=dst.at[c], send_sem=send.at[c], recv_sem=recv.at[c],
                                            device_id={"tp": peer}, device_id_type=pl.DeviceIdType.MESH)

    def to_partner(c, bufs):
        return remote(bufs[0], bufs[2], bufs[4], bufs[5], c, partner)

    def to_across(c, bufs):
        return remote(bufs[1], bufs[3], bufs[6], bufs[7], c, across)

    def relay(c, bufs):
        to_partner(c, bufs).wait_recv()
        bufs[1][c] = (bufs[0][c].astype(F32) + bufs[2][c].astype(F32)).astype(BF16)
        to_across(c, bufs).start()

    def finish(c, bufs):
        to_across(c, bufs).wait_recv()
        total[:, c * CHUNK:(c + 1) * CHUNK] = bufs[1][c].astype(F32) + bufs[3][c].astype(F32)

    def drain(bufs):
        for c in range(chunks):
            to_partner(c, bufs).wait_send()
            to_across(c, bufs).wait_send()

    obufs = (osend, ohalf, orecv1, orecv2, os1, or1, os2, or2)
    fbufs = (fsend, fhalf, frecv1, frecv2, fs1, fr1, fs2, fr2)

    small[0].wait()
    for c in range(chunks):
        to_partner(c, obufs).start()
    for c in range(chunks):
        relay(c, obufs)
    for copy in small[1:]:
        copy.wait()
    for c in range(chunks):
        finish(c, obufs)
    x1 = (x[...].astype(F32) + normed(total[...], gain[1:2, :]).astype(F32)).astype(BF16)
    x[...] = x1
    a = normed(x1.astype(F32), gain[2:3, :])

    for c in range(chunks):
        gates[c].wait()
        gate = jnp.dot(a, wg[c], preferred_element_type=F32)
        ups[c].wait()
        up = jnp.dot(a, wu[c], preferred_element_type=F32)
        h[:, c * CHUNK:(c + 1) * CHUNK] = (jax.nn.gelu(gate, approximate=True) * up).astype(BF16)
    act = h[...]
    for c in range(chunks):
        downs[c].wait()
        fsend[c] = jnp.dot(act, wd[c], preferred_element_type=F32).astype(BF16)
        to_partner(c, fbufs).start()
        if c >= 2:
            relay(c - 2, fbufs)
    for c in range(chunks - 2, chunks):
        relay(c, fbufs)
    for c in range(chunks):
        finish(c, fbufs)
    out_ref[...] = (x[...].astype(F32) + normed(total[...], gain[3:4, :]).astype(F32)).astype(BF16)
    drain(obufs)
    drain(fbufs)


def in_hbm(value):
    return pltpu.with_memory_space_constraint(value, pltpu.HBM)


def attn_call(layer, masked, pos, x, gains, freq, wq, wk, wv, wo, kc, vc):
    n = kc.shape[1]
    dma = pltpu.SemaphoreType.DMA
    any_spec = pl.BlockSpec(memory_space=pl.ANY)
    return pl.pallas_call(
        functools.partial(attn_kernel, layer, masked),
        name=f"attn{layer}",
        out_shape=(jax.ShapeDtypeStruct(kc.shape, BF16), jax.ShapeDtypeStruct(vc.shape, BF16),
                   jax.ShapeDtypeStruct((D // CHUNK, ROWS, CHUNK), BF16)),
        in_specs=[any_spec] * 10,
        out_specs=(pl.BlockSpec(memory_space=pltpu.HBM), pl.BlockSpec(memory_space=pltpu.HBM), pl.BlockSpec(memory_space=pltpu.VMEM)),
        scratch_shapes=[
            pltpu.SMEM((ROWS,), jnp.int32),
            pltpu.VMEM((ROWS, D), BF16), pltpu.VMEM((4, D), F32), pltpu.VMEM((1, HALF), F32),
            pltpu.VMEM((D, 2 * HEAD), BF16), pltpu.VMEM((D, HEAD), BF16), pltpu.VMEM((D, HEAD), BF16), pltpu.VMEM((2 * HEAD, D), BF16),
            pltpu.VMEM((SLOTS, GROUP, n, HEAD), BF16), pltpu.VMEM((SLOTS, GROUP, n, HEAD), BF16),
            pltpu.VMEM((2 * ROWS, HALF), F32), pltpu.VMEM((2 * ROWS, HALF), F32),
            pltpu.VMEM((2 * ROWS, HALF), F32), pltpu.VMEM((2 * ROWS, HALF), F32),
            pltpu.VMEM((ROWS, HEAD), F32), pltpu.VMEM((ROWS, HEAD), F32),
            dma((4,)), dma((4,)), dma((SLOTS,)), dma((SLOTS,)), dma((SLOTS,)), dma((SLOTS,)),
        ],
        compiler_params=pltpu.CompilerParams(vmem_limit_bytes=50 * 2 ** 20),
    )(pos, x, gains, freq, in_hbm(wq), in_hbm(wk), in_hbm(wv), in_hbm(wo), in_hbm(kc), in_hbm(vc))


def mlp_call(layer, x, o, gains, wg, wu, wd):
    dma = pltpu.SemaphoreType.DMA
    chunks = D // CHUNK
    any_spec = pl.BlockSpec(memory_space=pl.ANY)
    wide = pltpu.VMEM((chunks, D, CHUNK), BF16)
    piece = pltpu.VMEM((chunks, ROWS, CHUNK), BF16)
    return pl.pallas_call(
        functools.partial(mlp_kernel, layer),
        name=f"mlp{layer}",
        out_shape=jax.ShapeDtypeStruct((ROWS, D), BF16),
        in_specs=[any_spec] * 6,
        out_specs=pl.BlockSpec(memory_space=pltpu.VMEM),
        scratch_shapes=[
            pltpu.VMEM((ROWS, D), BF16), pltpu.VMEM((4, D), F32), wide, wide, wide, pltpu.VMEM((ROWS, D), BF16),
            piece, piece, piece, piece, piece, piece, piece, piece, pltpu.VMEM((ROWS, D), F32),
            dma((3,)), dma((chunks,)), dma((chunks,)), dma((chunks,)),
        ] + [dma((chunks,))] * 8,
        compiler_params=pltpu.CompilerParams(collective_id=layer, has_side_effects=True, vmem_limit_bytes=50 * 2 ** 20),
    )(x, o, gains, in_hbm(wg), in_hbm(wu), in_hbm(wd))


def decode_step(hidden, positions, k_local, v_local, k_global, v_global, w_query, w_key, w_value, w_out, w_gate, w_up, w_down, norm_scale):
    freq = jnp.asarray((ROPE_BASE ** (-2.0 * np.arange(HALF) / HEAD)).astype(np.float32).reshape(1, HALF))

    def flat(cache):
        return cache.reshape(cache.shape[0], cache.shape[1], HEAD)

    outs = []
    x = hidden
    for layer, (k, v) in enumerate(((k_local, v_local), (k_global, v_global))):
        k_new, v_new, o = attn_call(layer, layer == 1, positions, x, norm_scale, freq, w_query, w_key, w_value, w_out, flat(k), flat(v))
        x = mlp_call(layer, x, o, norm_scale, w_gate, w_up, w_down)
        outs += [k_new.reshape(k.shape), v_new.reshape(v.shape)]
    return (x, *outs)


def solution(mesh):
    row_spec = P('dp', None)
    cache_spec = P('dp', None, 'tp', None)
    col_split = P(None, None, 'tp')
    row_split = P(None, 'tp', None)
    in_specs = (row_spec, P('dp'), cache_spec, cache_spec, cache_spec, cache_spec, col_split, col_split, col_split, row_split, col_split, col_split, row_split, P())
    out_specs = (row_spec, cache_spec, cache_spec, cache_spec, cache_spec)
    return jax.shard_map(decode_step, mesh=mesh, in_specs=in_specs, out_specs=out_specs, check_vma=False)
```

```python
import functools

import jax
import jax.numpy as jnp
import numpy as np
from jax import lax
from jax.experimental import pallas as pl
from jax.experimental.pallas import tpu as pltpu
from jax.sharding import PartitionSpec as P

SOFT_CAP = 50.0
NORM_EPS = 1e-6
ROPE_BASE = 10000.0
ROWS = 24
D = 2560
HEAD = 256
HALF = 128
GROUP = 4
CHUNK = 512
SIDE = D // 2
MIB = 2 ** 20
F32 = jnp.float32
BF16 = jnp.bfloat16


def normed(values, gain_row):
    inv_rms = lax.rsqrt(jnp.mean(values * values, axis=-1, keepdims=True) + NORM_EPS)
    return (values * inv_rms * (1.0 + gain_row)).astype(BF16)


def rotation(pos, freq):
    row_ids = lax.broadcasted_iota(jnp.int32, (ROWS, HALF), 0)
    pos_rows = jnp.zeros((ROWS, HALF), jnp.int32)
    for b in range(ROWS):
        pos_rows = jnp.where(row_ids == b, pos[b], pos_rows)
    angles = pos_rows.astype(F32) * freq
    return jnp.cos(angles), jnp.sin(angles)


def rotate(t, cos_part, sin_part):
    first, second = t[:, :HALF], t[:, HALF:]
    return first * cos_part - second * sin_part, second * cos_part + first * sin_part


def store_queries(q, cos_part, sin_part, qa, qb):
    for h in range(2):
        first, second = rotate(q[:, h * HEAD:(h + 1) * HEAD], cos_part, sin_part)
        qa[pl.ds(h, ROWS, stride=2), :] = first
        qb[pl.ds(h, ROWS, stride=2), :] = second


def store_key(k, cos_part, sin_part, knew):
    first, second = rotate(k, cos_part, sin_part)
    knew[:, :HALF] = first
    knew[:, HALF:] = second


def patch(buf, j, row, b, new):
    base = pl.multiple_of((row // 16) * 16, 16)
    tile = buf[j, pl.ds(base, 16), :].astype(F32)
    hit = lax.broadcasted_iota(jnp.int32, (16, HEAD), 0) == row - base
    fresh = jnp.broadcast_to(new[pl.ds(b, 1), :], (16, HEAD))
    buf[j, pl.ds(base, 16), :] = jnp.where(hit, fresh, tile).astype(BF16)


def attend_group(masked, g, pos, kref, vref, wait_k, wait_v, qa, qb, ma, mb, knew, vnew):
    n = kref.shape[1]
    rows8 = pl.ds(g * 8 if isinstance(g, int) else pl.multiple_of(g * 8, 8), 8)
    wait_k()
    for j in range(GROUP):
        b = g * GROUP + j
        patch(kref, j, lax.rem(pos[b], n), b, knew)
    q8 = jnp.concatenate([qa[rows8, :], qb[rows8, :]], axis=1).astype(BF16)
    owner = lax.broadcasted_iota(jnp.int32, (8, n), 0) // 2
    s = None
    for j in range(GROUP):
        part = lax.dot_general(q8, kref[j], (((1,), (1,)), ((), ())), preferred_element_type=F32)
        s = part if s is None else jnp.where(owner == j, part, s)
    e = jnp.exp(SOFT_CAP * jnp.tanh(s * (HEAD ** -0.5 / SOFT_CAP)))
    if masked:
        limit_rows = lax.broadcasted_iota(jnp.int32, (8, 1), 0) // 2
        limit = jnp.zeros((8, 1), jnp.int32)
        for j in range(GROUP):
            limit = jnp.where(limit_rows == j, pos[g * GROUP + j], limit)
        e = jnp.where(lax.broadcasted_iota(jnp.int32, (8, n), 1) <= limit, e, 0.0)
    p = (e / jnp.sum(e, axis=-1, keepdims=True)).astype(BF16)
    wait_v()
    for j in range(GROUP):
        b = g * GROUP + j
        patch(vref, j, lax.rem(pos[b], n), b, vnew)
    owner = lax.broadcasted_iota(jnp.int32, (8, HEAD), 0) // 2
    m = None
    for j in range(GROUP):
        part = jnp.dot(p, vref[j], preferred_element_type=F32)
        m = part if m is None else jnp.where(owner == j, part, m)
    ma[rows8, :] = m[:, :HALF]
    mb[rows8, :] = m[:, HALF:]


def project_out(ma, mb, wo, o_ref):
    mixed = jnp.concatenate([ref[pl.ds(h, ROWS, stride=2), :] for h in range(2) for ref in (ma, mb)], axis=1).astype(BF16)
    for c in range(2):
        o_ref[c] = jnp.dot(mixed, wo[:, c * SIDE:(c + 1) * SIDE], preferred_element_type=F32).astype(BF16)


def group_rows(ref, g):
    return ref.at[pl.ds(g * GROUP, GROUP)]


def local_kernel(pos_hbm, x_hbm, gain_hbm, freq_hbm, wq_hbm, wk_hbm, wv_hbm, wo_hbm, kc_hbm, vc_hbm,
                 ko_hbm, vo_hbm, o_ref, cos_ref, sin_ref,
                 pos, x, gain, freq, wq, wk, wv, wo, kbuf, vbuf, qa, qb, ma, mb, knew, vnew,
                 small_sem, w_sem, kr_sem, vr_sem, kw_sem, vw_sem):
    groups = ROWS // GROUP
    small = [pltpu.make_async_copy(s, d, small_sem.at[i]) for i, (s, d) in enumerate(
        ((x_hbm, x), (gain_hbm.at[0], gain), (pos_hbm, pos), (freq_hbm, freq)))]
    weights = [pltpu.make_async_copy(s.at[0], d, w_sem.at[i]) for i, (s, d) in enumerate(
        ((wq_hbm, wq), (wk_hbm, wk), (wv_hbm, wv), (wo_hbm, wo)))]

    def k_read(g):
        return pltpu.make_async_copy(group_rows(kc_hbm, g), kbuf.at[g], kr_sem.at[g])

    def v_read(g):
        return pltpu.make_async_copy(group_rows(vc_hbm, g), vbuf.at[g], vr_sem.at[g])

    def writes(g):
        return (pltpu.make_async_copy(kbuf.at[g], group_rows(ko_hbm, g), kw_sem.at[g]),
                pltpu.make_async_copy(vbuf.at[g], group_rows(vo_hbm, g), vw_sem.at[g]))

    for copy in small + weights[:3]:
        copy.start()
    for g in range(groups):
        k_read(g).start()
        v_read(g).start()
    weights[3].start()

    for copy in small:
        copy.wait()
    cos_part, sin_part = rotation(pos, freq[...])
    cos_ref[...] = cos_part
    sin_ref[...] = sin_part
    a = normed(x[...].astype(F32), gain[0:1, :])
    weights[0].wait()
    store_queries(jnp.dot(a, wq[...], preferred_element_type=F32), cos_part, sin_part, qa, qb)
    weights[1].wait()
    store_key(jnp.dot(a, wk[...], preferred_element_type=F32), cos_part, sin_part, knew)
    weights[2].wait()
    vnew[...] = jnp.dot(a, wv[...], preferred_element_type=F32)

    def step(g, carry):
        attend_group(False, g, pos, kbuf.at[g], vbuf.at[g], lambda: k_read(g).wait(), lambda: v_read(g).wait(), qa, qb, ma, mb, knew, vnew)
        for copy in writes(g):
            copy.start()
        return carry

    lax.fori_loop(0, groups, step, 0)
    weights[3].wait()
    project_out(ma, mb, wo, o_ref)
    for g in range(groups):
        for copy in writes(g):
            copy.wait()


def global_kernel(pos_hbm, a_ref, cos_ref, sin_ref, wq, wk, wv, wo, _k_first, _v_first, kc_hbm, vc_hbm,
                  ko_hbm, vo_hbm, o_ref, kfirst, vfirst,
                  pos, kbuf, vbuf, qa, qb, ma, mb, knew, vnew,
                  pos_sem, kr_sem, vr_sem, kw_sem, vw_sem):
    groups = ROWS // GROUP
    pos_copy = pltpu.make_async_copy(pos_hbm, pos, pos_sem)

    def k_read(g):
        return pltpu.make_async_copy(group_rows(kc_hbm, g), kbuf.at[g - 1], kr_sem.at[g - 1])

    def v_read(g):
        return pltpu.make_async_copy(group_rows(vc_hbm, g), vbuf.at[g - 1], vr_sem.at[g - 1])

    def writes(g, k, v):
        return (pltpu.make_async_copy(k, group_rows(ko_hbm, g), kw_sem.at[g]),
                pltpu.make_async_copy(v, group_rows(vo_hbm, g), vw_sem.at[g]))

    pos_copy.start()
    for g in range(1, groups):
        k_read(g).start()
        v_read(g).start()
    cos_part, sin_part = cos_ref[...], sin_ref[...]
    a = a_ref[...]
    store_queries(jnp.dot(a, wq[...], preferred_element_type=F32), cos_part, sin_part, qa, qb)
    store_key(jnp.dot(a, wk[...], preferred_element_type=F32), cos_part, sin_part, knew)
    vnew[...] = jnp.dot(a, wv[...], preferred_element_type=F32)
    pos_copy.wait()

    attend_group(True, 0, pos, kfirst, vfirst, lambda: None, lambda: None, qa, qb, ma, mb, knew, vnew)
    for copy in writes(0, kfirst, vfirst):
        copy.start()

    def step(g, carry):
        k, v = kbuf.at[g - 1], vbuf.at[g - 1]
        attend_group(True, g, pos, k, v, lambda: k_read(g).wait(), lambda: v_read(g).wait(), qa, qb, ma, mb, knew, vnew)
        for copy in writes(g, k, v):
            copy.start()
        return carry

    lax.fori_loop(1, groups, step, 0)
    project_out(ma, mb, wo, o_ref)
    for copy in writes(0, kfirst, vfirst):
        copy.wait()
    for g in range(1, groups):
        for copy in writes(g, kbuf.at[g - 1], vbuf.at[g - 1]):
            copy.wait()


def mlp_kernel(layer, *refs):
    n_in, n_out = (12, 8) if layer == 0 else (6, 1)
    x_hbm, o_ref, gain_hbm, wg_hbm, wu_hbm, wd_hbm = refs[:6]
    outs = refs[n_in:n_in + n_out]
    (x, gain, wg, wu, wd, h, osend, ohalf, orecv1, orecv2, osum, fsend, fhalf, frecv1, frecv2, total,
     small_sem, g_sem, u_sem, d_sem, ahead_sem, o_send, o_recv, fs1, fr1, fs2, fr2) = refs[n_in + n_out:]
    out_ref = outs[0]
    chunks = D // CHUNK
    me = lax.axis_index("tp")
    chip, core = me // 2, lax.rem(me, 2)
    partner = chip * 2 + (1 - core)
    across = (1 - chip) * 2 + core

    small = [pltpu.make_async_copy(s, d, small_sem.at[i]) for i, (s, d) in enumerate(
        ((o_ref, osend), (x_hbm, x), (gain_hbm, gain)))]
    cols = [pl.ds(c * CHUNK, CHUNK) for c in range(chunks)]
    gates = [pltpu.make_async_copy(wg_hbm.at[layer, :, cols[c]], wg.at[c], g_sem.at[c]) for c in range(chunks)]
    ups = [pltpu.make_async_copy(wu_hbm.at[layer, :, cols[c]], wu.at[c], u_sem.at[c]) for c in range(chunks)]
    downs = [pltpu.make_async_copy(wd_hbm.at[layer, :, cols[c]], wd.at[c], d_sem.at[c]) for c in range(chunks)]
    for copy in small:
        copy.start()
    for c in range(chunks):
        gates[c].start()
        ups[c].start()
    for c in range(chunks):
        downs[c].start()
    ahead = []
    if layer == 0:
        wq_hbm, wk_hbm, wv_hbm, wo_hbm, kc_hbm, vc_hbm = refs[6:12]
        sources = [w.at[1] for w in (wq_hbm, wk_hbm, wv_hbm, wo_hbm)] + [group_rows(kc_hbm, 0), group_rows(vc_hbm, 0)]
        ahead = [pltpu.make_async_copy(s, d, ahead_sem.at[i]) for i, (s, d) in enumerate(zip(sources, outs[2:]))]
        for copy in ahead:
            copy.start(priority=1)

    barrier = pltpu.get_barrier_semaphore()
    for peer in (partner, across):
        pl.semaphore_signal(barrier, inc=1, device_id={"tp": peer}, device_id_type=pl.DeviceIdType.MESH)
    pl.semaphore_wait(barrier, 2)

    def remote(src, dst, send, recv, peer):
        return pltpu.make_async_remote_copy(src_ref=src, dst_ref=dst, send_sem=send, recv_sem=recv,
                                            device_id={"tp": peer}, device_id_type=pl.DeviceIdType.MESH)

    o_copies = (remote(osend.at[1 - core], orecv1, o_send.at[0], o_recv.at[0], partner),
                remote(ohalf, orecv2, o_send.at[1], o_recv.at[1], across),
                remote(osum.at[core], osum.at[core], o_send.at[2], o_recv.at[2], partner))
    small[0].wait()
    o_copies[0].start()
    for copy in small[1:]:
        copy.wait()
    o_copies[0].wait_recv()
    ohalf[...] = (osend[core].astype(F32) + orecv1[...].astype(F32)).astype(BF16)
    o_copies[1].start()
    o_copies[1].wait_recv()
    osum[core] = (ohalf[...].astype(F32) + orecv2[...].astype(F32)).astype(BF16)
    o_copies[2].start()
    o_copies[2].wait_recv()
    o_sum = jnp.concatenate([osum[0], osum[1]], axis=1).astype(F32)
    x1 = (x[...].astype(F32) + normed(o_sum, gain[layer, 1:2, :]).astype(F32)).astype(BF16)
    x[...] = x1
    a = normed(x1.astype(F32), gain[layer, 2:3, :])

    for c in range(chunks):
        gates[c].wait()
        gate = jnp.dot(a, wg[c], preferred_element_type=F32)
        ups[c].wait()
        up = jnp.dot(a, wu[c], preferred_element_type=F32)
        h[:, c * CHUNK:(c + 1) * CHUNK] = (jax.nn.gelu(gate, approximate=True) * up).astype(BF16)
    act = h[...]

    def to_partner(c):
        return remote(fsend.at[c], frecv1.at[c], fs1.at[c], fr1.at[c], partner)

    def to_across(c):
        return remote(fhalf.at[c], frecv2.at[c], fs2.at[c], fr2.at[c], across)

    def relay(c):
        to_partner(c).wait_recv()
        fhalf[c] = (fsend[c].astype(F32) + frecv1[c].astype(F32)).astype(BF16)
        to_across(c).start()

    for c in range(chunks):
        downs[c].wait()
        fsend[c] = jnp.dot(act, wd[c], preferred_element_type=F32).astype(BF16)
        to_partner(c).start()
        if c >= 3:
            relay(c - 3)
    for c in range(chunks - 3, chunks):
        relay(c)
    squares = jnp.zeros((ROWS, HALF), F32)
    for c in range(chunks):
        to_across(c).wait_recv()
        piece = fhalf[c].astype(F32) + frecv2[c].astype(F32)
        total[:, c * CHUNK:(c + 1) * CHUNK] = piece
        for i in range(CHUNK // HALF):
            lane_block = piece[:, i * HALF:(i + 1) * HALF]
            squares = squares + lane_block * lane_block
    inv_rms = lax.rsqrt(jnp.sum(squares, axis=-1, keepdims=True) / D + NORM_EPS)
    branch = (total[...] * inv_rms * (1.0 + gain[layer, 3:4, :])).astype(BF16)
    x2 = (x[...].astype(F32) + branch.astype(F32)).astype(BF16)
    out_ref[...] = x2
    if layer == 0:
        outs[1][...] = normed(x2.astype(F32), gain[1, 0:1, :])
    for copy in o_copies:
        copy.wait_send()
    for c in range(chunks):
        to_partner(c).wait_send()
        to_across(c).wait_send()
    for copy in ahead:
        copy.wait()


def in_hbm(value):
    return pltpu.with_memory_space_constraint(value, pltpu.HBM)


def in_vmem(value):
    return pltpu.with_memory_space_constraint(value, pltpu.VMEM)


ANY = pl.BlockSpec(memory_space=pl.ANY)
IN_HBM = pl.BlockSpec(memory_space=pltpu.HBM)
IN_VMEM = pl.BlockSpec(memory_space=pltpu.VMEM)
DMA = pltpu.SemaphoreType.DMA


def head_scratch():
    return [pltpu.VMEM((2 * ROWS, HALF), F32)] * 4 + [pltpu.VMEM((ROWS, HEAD), F32)] * 2


def local_call(pos, x, gains, freq, wq, wk, wv, wo, kc, vc):
    groups, n = ROWS // GROUP, kc.shape[1]
    table = pltpu.VMEM((ROWS, HALF), F32)
    return pl.pallas_call(
        local_kernel,
        name="local_attention",
        out_shape=(jax.ShapeDtypeStruct(kc.shape, BF16), jax.ShapeDtypeStruct(vc.shape, BF16),
                   pltpu.VMEM((2, ROWS, SIDE), BF16), table, table),
        in_specs=[ANY] * 10,
        out_specs=(IN_HBM, IN_HBM, IN_VMEM, IN_VMEM, IN_VMEM),
        scratch_shapes=[
            pltpu.SMEM((ROWS,), jnp.int32),
            pltpu.VMEM((ROWS, D), BF16), pltpu.VMEM((4, D), F32), pltpu.VMEM((1, HALF), F32),
            pltpu.VMEM((D, 2 * HEAD), BF16), pltpu.VMEM((D, HEAD), BF16), pltpu.VMEM((D, HEAD), BF16), pltpu.VMEM((2 * HEAD, D), BF16),
            pltpu.VMEM((groups, GROUP, n, HEAD), BF16), pltpu.VMEM((groups, GROUP, n, HEAD), BF16),
        ] + head_scratch() + [DMA((4,)), DMA((4,))] + [DMA((groups,))] * 4,
        compiler_params=pltpu.CompilerParams(vmem_limit_bytes=40 * MIB),
    )(*[in_hbm(v) for v in (pos, x, gains, freq, wq, wk, wv, wo, kc, vc)])


def global_call(pos, a, cos_part, sin_part, ahead, kc, vc):
    groups, n = ROWS // GROUP, kc.shape[1]
    first = pltpu.VMEM((GROUP, n, HEAD), BF16)
    return pl.pallas_call(
        global_kernel,
        name="global_attention",
        out_shape=(jax.ShapeDtypeStruct(kc.shape, BF16), jax.ShapeDtypeStruct(vc.shape, BF16),
                   pltpu.VMEM((2, ROWS, SIDE), BF16), first, first),
        in_specs=[ANY] + [IN_VMEM] * 9 + [ANY] * 2,
        out_specs=(IN_HBM, IN_HBM, IN_VMEM, IN_VMEM, IN_VMEM),
        input_output_aliases={8: 3, 9: 4},
        scratch_shapes=[
            pltpu.SMEM((ROWS,), jnp.int32),
            pltpu.VMEM((groups - 1, GROUP, n, HEAD), BF16), pltpu.VMEM((groups - 1, GROUP, n, HEAD), BF16),
        ] + head_scratch() + [DMA(())] + [DMA((groups - 1,))] * 2 + [DMA((groups,))] * 2,
        compiler_params=pltpu.CompilerParams(vmem_limit_bytes=42 * MIB),
    )(in_hbm(pos), *[in_vmem(v) for v in (a, cos_part, sin_part, *ahead)], in_hbm(kc), in_hbm(vc))


def mlp_call(layer, x, o, gains, wg, wu, wd, ahead=()):
    chunks = D // CHUNK
    wide = pltpu.VMEM((chunks, D, CHUNK), BF16)
    piece = pltpu.VMEM((chunks, ROWS, CHUNK), BF16)
    side = pltpu.VMEM((ROWS, SIDE), BF16)
    both = pltpu.VMEM((2, ROWS, SIDE), BF16)
    rows = pltpu.VMEM((ROWS, D), BF16)
    out_shape = [rows]
    if ahead:
        out_shape += [rows] + [pltpu.VMEM(w.shape[1:], BF16) for w in ahead[:4]]
        out_shape += [pltpu.VMEM((GROUP,) + c.shape[1:], BF16) for c in ahead[4:]]
    return pl.pallas_call(
        functools.partial(mlp_kernel, layer),
        name=f"mlp{layer}",
        out_shape=out_shape,
        in_specs=[ANY] * (6 + len(ahead)),
        out_specs=[IN_VMEM] * len(out_shape),
        scratch_shapes=[
            pltpu.VMEM((ROWS, D), BF16), pltpu.VMEM((2, 4, D), F32), wide, wide, wide, pltpu.VMEM((ROWS, D), BF16),
            both, side, side, side, both, piece, piece, piece, piece, pltpu.VMEM((ROWS, D), F32),
            DMA((3,)), DMA((chunks,)), DMA((chunks,)), DMA((chunks,)), DMA((6,)), DMA((3,)), DMA((3,)),
        ] + [DMA((chunks,))] * 4,
        compiler_params=pltpu.CompilerParams(collective_id=layer, has_side_effects=True, vmem_limit_bytes=40 * MIB),
    )(x, in_vmem(o), *[in_hbm(v) for v in (gains, wg, wu, wd) + tuple(ahead)])


def decode_step(hidden, positions, k_local, v_local, k_global, v_global, w_query, w_key, w_value, w_out, w_gate, w_up, w_down, norm_scale):
    freq = jnp.asarray((ROPE_BASE ** (-2.0 * np.arange(HALF) / HEAD)).astype(np.float32).reshape(1, HALF))

    def flat(cache):
        return cache.reshape(cache.shape[0], cache.shape[1], HEAD)

    kg, vg = flat(k_global), flat(v_global)
    kl_new, vl_new, o, cos_part, sin_part = local_call(positions, hidden, norm_scale, freq, w_query, w_key, w_value, w_out, flat(k_local), flat(v_local))
    x, a, *ahead = mlp_call(0, in_hbm(hidden), o, norm_scale, w_gate, w_up, w_down, (w_query, w_key, w_value, w_out, kg, vg))
    kg_new, vg_new, o, _, _ = global_call(positions, a, cos_part, sin_part, ahead, kg, vg)
    (x,) = mlp_call(1, in_vmem(x), o, norm_scale, w_gate, w_up, w_down)
    return (x, kl_new.reshape(k_local.shape), vl_new.reshape(v_local.shape), kg_new.reshape(k_global.shape), vg_new.reshape(v_global.shape))


def solution(mesh):
    row_spec = P('dp', None)
    cache_spec = P('dp', None, 'tp', None)
    col_split = P(None, None, 'tp')
    row_split = P(None, 'tp', None)
    in_specs = (row_spec, P('dp'), cache_spec, cache_spec, cache_spec, cache_spec, col_split, col_split, col_split, row_split, col_split, col_split, row_split, P())
    out_specs = (row_spec, cache_spec, cache_spec, cache_spec, cache_spec)
    return jax.shard_map(decode_step, mesh=mesh, in_specs=in_specs, out_specs=out_specs, check_vma=False)
```

```python
import functools

import jax
import jax.numpy as jnp
import numpy as np
from jax import lax
from jax.experimental import pallas as pl
from jax.experimental.pallas import tpu as pltpu
from jax.sharding import PartitionSpec as P

SOFT_CAP = 50.0
NORM_EPS = 1e-6
ROPE_BASE = 10000.0
ROWS = 24
D = 2560
HEAD = 256
HALF = 128
GROUP = 4
CHUNK = 512
SIDE = D // 2
MIB = 2 ** 20
WIDE = ((0, 1536), (1536, 1024))
DOWN = ((0, 1280), (1280, 768), (2048, 512))
F32 = jnp.float32
BF16 = jnp.bfloat16


def normed(values, gain_row):
    inv_rms = lax.rsqrt(jnp.mean(values * values, axis=-1, keepdims=True) + NORM_EPS)
    return (values * inv_rms * (1.0 + gain_row)).astype(BF16)


def rotation(pos, freq):
    row_ids = lax.broadcasted_iota(jnp.int32, (ROWS, HALF), 0)
    pos_rows = jnp.zeros((ROWS, HALF), jnp.int32)
    for b in range(ROWS):
        pos_rows = jnp.where(row_ids == b, pos[b], pos_rows)
    angles = pos_rows.astype(F32) * freq
    return jnp.cos(angles), jnp.sin(angles)


def rotate(t, cos_part, sin_part):
    first, second = t[:, :HALF], t[:, HALF:]
    return first * cos_part - second * sin_part, second * cos_part + first * sin_part


def store_queries(q, cos_part, sin_part, qa, qb):
    for h in range(2):
        first, second = rotate(q[:, h * HEAD:(h + 1) * HEAD], cos_part, sin_part)
        qa[pl.ds(h, ROWS, stride=2), :] = first
        qb[pl.ds(h, ROWS, stride=2), :] = second


def store_key(k, cos_part, sin_part, knew):
    first, second = rotate(k, cos_part, sin_part)
    knew[:, :HALF] = first
    knew[:, HALF:] = second


def patch(buf, j, row, b, new):
    base = pl.multiple_of((row // 16) * 16, 16)
    tile = buf[j, pl.ds(base, 16), :].astype(F32)
    hit = lax.broadcasted_iota(jnp.int32, (16, HEAD), 0) == row - base
    fresh = jnp.broadcast_to(new[pl.ds(b, 1), :], (16, HEAD))
    buf[j, pl.ds(base, 16), :] = jnp.where(hit, fresh, tile).astype(BF16)


def attend_group(masked, g, pos, kref, vref, wait_k, wait_v, qa, qb, ma, mb, knew, vnew):
    n = kref.shape[1]
    rows8 = pl.ds(g * 8 if isinstance(g, int) else pl.multiple_of(g * 8, 8), 8)
    wait_k()
    for j in range(GROUP):
        b = g * GROUP + j
        patch(kref, j, lax.rem(pos[b], n), b, knew)
    q8 = jnp.concatenate([qa[rows8, :], qb[rows8, :]], axis=1).astype(BF16)
    owner = lax.broadcasted_iota(jnp.int32, (8, n), 0) // 2
    s = None
    for j in range(GROUP):
        part = lax.dot_general(q8, kref[j], (((1,), (1,)), ((), ())), preferred_element_type=F32)
        s = part if s is None else jnp.where(owner == j, part, s)
    e = jnp.exp(SOFT_CAP * jnp.tanh(s * (HEAD ** -0.5 / SOFT_CAP)))
    if masked:
        limit_rows = lax.broadcasted_iota(jnp.int32, (8, 1), 0) // 2
        limit = jnp.zeros((8, 1), jnp.int32)
        for j in range(GROUP):
            limit = jnp.where(limit_rows == j, pos[g * GROUP + j], limit)
        e = jnp.where(lax.broadcasted_iota(jnp.int32, (8, n), 1) <= limit, e, 0.0)
    p = (e / jnp.sum(e, axis=-1, keepdims=True)).astype(BF16)
    wait_v()
    for j in range(GROUP):
        b = g * GROUP + j
        patch(vref, j, lax.rem(pos[b], n), b, vnew)
    owner = lax.broadcasted_iota(jnp.int32, (8, HEAD), 0) // 2
    m = None
    for j in range(GROUP):
        part = jnp.dot(p, vref[j], preferred_element_type=F32)
        m = part if m is None else jnp.where(owner == j, part, m)
    ma[rows8, :] = m[:, :HALF]
    mb[rows8, :] = m[:, HALF:]


def project_out(ma, mb, wo, o_ref):
    mixed = jnp.concatenate([ref[pl.ds(h, ROWS, stride=2), :] for h in range(2) for ref in (ma, mb)], axis=1).astype(BF16)
    for c in range(2):
        o_ref[c] = jnp.dot(mixed, wo[:, c * SIDE:(c + 1) * SIDE], preferred_element_type=F32).astype(BF16)


def group_rows(ref, g):
    return ref.at[pl.ds(g * GROUP, GROUP)]


def local_kernel(pos_hbm, x_hbm, gain_hbm, freq_hbm, wq_hbm, wk_hbm, wv_hbm, wo_hbm, kc_hbm, vc_hbm,
                 ko_hbm, vo_hbm, o_ref, cos_ref, sin_ref, x,
                 pos, gain, freq, wq, wk, wv, wo, kbuf, vbuf, qa, qb, ma, mb, knew, vnew,
                 small_sem, w_sem, kr_sem, vr_sem, kw_sem, vw_sem):
    groups = ROWS // GROUP
    small = [pltpu.make_async_copy(s, d, small_sem.at[i]) for i, (s, d) in enumerate(
        ((x_hbm, x), (gain_hbm.at[0], gain), (pos_hbm, pos), (freq_hbm, freq)))]
    weights = [pltpu.make_async_copy(s.at[0], d, w_sem.at[i]) for i, (s, d) in enumerate(
        ((wq_hbm, wq), (wk_hbm, wk), (wv_hbm, wv), (wo_hbm, wo)))]

    def k_read(g):
        return pltpu.make_async_copy(group_rows(kc_hbm, g), kbuf.at[g], kr_sem.at[g])

    def v_read(g):
        return pltpu.make_async_copy(group_rows(vc_hbm, g), vbuf.at[g], vr_sem.at[g])

    def writes(g):
        return (pltpu.make_async_copy(kbuf.at[g], group_rows(ko_hbm, g), kw_sem.at[g]),
                pltpu.make_async_copy(vbuf.at[g], group_rows(vo_hbm, g), vw_sem.at[g]))

    for copy in small:
        copy.start()
    for copy in weights[:3]:
        copy.start(priority=1)
    for g in range(groups):
        k_read(g).start(priority=1)
        v_read(g).start(priority=1)
    weights[3].start(priority=1)

    for copy in small:
        copy.wait()
    cos_part, sin_part = rotation(pos, freq[...])
    cos_ref[...] = cos_part
    sin_ref[...] = sin_part
    a = normed(x[...].astype(F32), gain[0:1, :])
    weights[0].wait()
    store_queries(jnp.dot(a, wq[...], preferred_element_type=F32), cos_part, sin_part, qa, qb)
    weights[1].wait()
    store_key(jnp.dot(a, wk[...], preferred_element_type=F32), cos_part, sin_part, knew)
    weights[2].wait()
    vnew[...] = jnp.dot(a, wv[...], preferred_element_type=F32)

    def step(g, carry):
        attend_group(False, g, pos, kbuf.at[g], vbuf.at[g], lambda: k_read(g).wait(), lambda: v_read(g).wait(), qa, qb, ma, mb, knew, vnew)
        for copy in writes(g):
            copy.start(priority=1)
        return carry

    lax.fori_loop(0, groups, step, 0)
    weights[3].wait()
    project_out(ma, mb, wo, o_ref)
    for g in range(groups):
        for copy in writes(g):
            copy.wait()


def global_kernel(pos_hbm, a_ref, cos_ref, sin_ref, wq, wk, wv, wo, _k_first, _v_first, kc_hbm, vc_hbm,
                  ko_hbm, vo_hbm, o_ref, kfirst, vfirst,
                  pos, kbuf, vbuf, qa, qb, ma, mb, knew, vnew,
                  pos_sem, kr_sem, vr_sem, kw_sem, vw_sem):
    groups = ROWS // GROUP
    pos_copy = pltpu.make_async_copy(pos_hbm, pos, pos_sem)

    def k_read(g):
        return pltpu.make_async_copy(group_rows(kc_hbm, g), kbuf.at[g - 1], kr_sem.at[g - 1])

    def v_read(g):
        return pltpu.make_async_copy(group_rows(vc_hbm, g), vbuf.at[g - 1], vr_sem.at[g - 1])

    def writes(g, k, v):
        return (pltpu.make_async_copy(k, group_rows(ko_hbm, g), kw_sem.at[g]),
                pltpu.make_async_copy(v, group_rows(vo_hbm, g), vw_sem.at[g]))

    def start_writes(g):
        for copy in writes(g, kfirst if g == 0 else kbuf.at[g - 1], vfirst if g == 0 else vbuf.at[g - 1]):
            copy.start(priority=1)

    pos_copy.start()
    for g in range(1, groups):
        k_read(g).start(priority=1)
        v_read(g).start(priority=1)
    cos_part, sin_part = cos_ref[...], sin_ref[...]
    a = a_ref[...]
    store_queries(jnp.dot(a, wq[...], preferred_element_type=F32), cos_part, sin_part, qa, qb)
    store_key(jnp.dot(a, wk[...], preferred_element_type=F32), cos_part, sin_part, knew)
    vnew[...] = jnp.dot(a, wv[...], preferred_element_type=F32)
    pos_copy.wait()

    attend_group(True, 0, pos, kfirst, vfirst, lambda: None, lambda: None, qa, qb, ma, mb, knew, vnew)

    def step(g, carry):
        k, v = kbuf.at[g - 1], vbuf.at[g - 1]

        def wait_v():
            v_read(g).wait()

            @pl.when(g == groups - 1)
            def _():
                for i in range(groups - 1):
                    start_writes(i)

        attend_group(True, g, pos, k, v, lambda: k_read(g).wait(), wait_v, qa, qb, ma, mb, knew, vnew)
        return carry

    lax.fori_loop(1, groups, step, 0)
    start_writes(groups - 1)
    project_out(ma, mb, wo, o_ref)
    for copy in writes(0, kfirst, vfirst):
        copy.wait()
    for g in range(1, groups):
        for copy in writes(g, kbuf.at[g - 1], vbuf.at[g - 1]):
            copy.wait()


def mlp_kernel(layer, *refs):
    n_in, n_out = (12, 8) if layer == 0 else (6, 1)
    x_ref, o_ref, gain_hbm, wg_hbm, wu_hbm, wd_hbm = refs[:6]
    outs = refs[n_in:n_in + n_out]
    (x, gain, wg, wu, wd, h, ohalf, orecv1, orecv2, osum, fsend, fhalf, frecv1, frecv2, total,
     small_sem, g_sem, u_sem, d_sem, ahead_sem, o_send, o_recv, fs1, fr1, fs2, fr2) = refs[n_in + n_out:]
    out_ref = outs[0]
    last = len(DOWN)
    me = lax.axis_index("tp")
    chip, core = me // 2, lax.rem(me, 2)
    partner = chip * 2 + (1 - core)
    across = (1 - chip) * 2 + (1 - core)
    side = lax.rem(chip + core, 2)

    gain_copy = pltpu.make_async_copy(gain_hbm, gain, small_sem)
    wide_cols = [pl.ds(start, size) for start, size in WIDE]
    down_cols = [pl.ds(start, size) for start, size in DOWN]
    gates = [pltpu.make_async_copy(wg_hbm.at[layer, :, d], wg.at[:, d], g_sem.at[i]) for i, d in enumerate(wide_cols)]
    ups = [pltpu.make_async_copy(wu_hbm.at[layer, :, d], wu.at[:, d], u_sem.at[i]) for i, d in enumerate(wide_cols)]
    downs = [pltpu.make_async_copy(wd_hbm.at[layer, :, d], wd.at[:, d], d_sem.at[i]) for i, d in enumerate(down_cols)]
    ahead = []
    if layer == 0:
        wq_hbm, wk_hbm, wv_hbm, wo_hbm, kc_hbm, vc_hbm = refs[6:12]
        sources = [w.at[1] for w in (wq_hbm, wk_hbm, wv_hbm, wo_hbm)] + [group_rows(kc_hbm, 0), group_rows(vc_hbm, 0)]
        ahead = [pltpu.make_async_copy(s, d, ahead_sem.at[i]) for i, (s, d) in enumerate(zip(sources, outs[2:]))]

    def start_bulk(copies):
        for copy in copies:
            copy.start(priority=1)

    gain_copy.start()
    start_bulk((gates[0], ups[0]))

    barrier = pltpu.get_barrier_semaphore()
    for peer in (partner, across):
        pl.semaphore_signal(barrier, inc=1, device_id={"tp": peer}, device_id_type=pl.DeviceIdType.MESH)
    pl.semaphore_wait(barrier, 2)

    def remote(src, dst, send, recv, peer):
        return pltpu.make_async_remote_copy(src_ref=src, dst_ref=dst, send_sem=send, recv_sem=recv,
                                            device_id={"tp": peer}, device_id_type=pl.DeviceIdType.MESH)

    o_copies = (remote(o_ref.at[1 - side], orecv1, o_send.at[0], o_recv.at[0], partner),
                remote(ohalf, orecv2, o_send.at[1], o_recv.at[1], across),
                remote(osum.at[side], osum.at[side], o_send.at[2], o_recv.at[2], partner))
    o_copies[0].start()
    start_bulk((gates[1], ups[1]))
    gain_copy.wait()
    o_copies[0].wait_recv()
    ohalf[...] = (o_ref[side].astype(F32) + orecv1[...].astype(F32)).astype(BF16)
    o_copies[1].start()
    o_copies[1].wait_recv()
    osum[side] = (ohalf[...].astype(F32) + orecv2[...].astype(F32)).astype(BF16)
    o_copies[2].start()
    o_copies[2].wait_recv()
    o_sum = jnp.concatenate([osum[0], osum[1]], axis=1).astype(F32)
    x1 = (x_ref[...].astype(F32) + normed(o_sum, gain[layer, 1:2, :]).astype(F32)).astype(BF16)
    x[...] = x1
    a = normed(x1.astype(F32), gain[layer, 2:3, :])

    for w, (start, size) in enumerate(WIDE):
        gates[w].wait()
        ups[w].wait()
        start_bulk(downs if w == 0 else ahead)
        for c in range(start, start + size, CHUNK):
            gate = jnp.dot(a, wg[:, c:c + CHUNK], preferred_element_type=F32)
            up = jnp.dot(a, wu[:, c:c + CHUNK], preferred_element_type=F32)
            h[:, c:c + CHUNK] = (jax.nn.gelu(gate, approximate=True) * up).astype(BF16)
    act = h[...]

    def to_partner(c):
        d = down_cols[c]
        return remote(fsend.at[:, d], frecv1.at[:, d], fs1.at[c], fr1.at[c], partner)

    def to_across(c):
        d = down_cols[c]
        return remote(fhalf.at[:, d], frecv2.at[:, d], fs2.at[c], fr2.at[c], across)

    def relay(c):
        d = down_cols[c]
        to_partner(c).wait_recv()
        fhalf[:, d] = (fsend[:, d].astype(F32) + frecv1[:, d].astype(F32)).astype(BF16)
        to_across(c).start()

    for c in range(last):
        downs[c].wait()
        fsend[:, down_cols[c]] = jnp.dot(act, wd[:, down_cols[c]], preferred_element_type=F32).astype(BF16)
        to_partner(c).start()
        if c >= 1:
            relay(c - 1)
    for c in range(last - 1, last):
        relay(c)
    squares = jnp.zeros((ROWS, HALF), F32)
    for c in range(last):
        to_across(c).wait_recv()
        piece = fhalf[:, down_cols[c]].astype(F32) + frecv2[:, down_cols[c]].astype(F32)
        total[:, down_cols[c]] = piece
        for i in range(DOWN[c][1] // HALF):
            lane_block = piece[:, i * HALF:(i + 1) * HALF]
            squares = squares + lane_block * lane_block
    inv_rms = lax.rsqrt(jnp.sum(squares, axis=-1, keepdims=True) / D + NORM_EPS)
    branch = (total[...] * inv_rms * (1.0 + gain[layer, 3:4, :])).astype(BF16)
    x2 = (x[...].astype(F32) + branch.astype(F32)).astype(BF16)
    out_ref[...] = x2
    if layer == 0:
        outs[1][...] = normed(x2.astype(F32), gain[1, 0:1, :])
    for copy in o_copies:
        copy.wait_send()
    for c in range(last):
        to_partner(c).wait_send()
        to_across(c).wait_send()
    for copy in ahead:
        copy.wait()


def in_hbm(value):
    return pltpu.with_memory_space_constraint(value, pltpu.HBM)


def in_vmem(value):
    return pltpu.with_memory_space_constraint(value, pltpu.VMEM)


ANY = pl.BlockSpec(memory_space=pl.ANY)
IN_HBM = pl.BlockSpec(memory_space=pltpu.HBM)
IN_VMEM = pl.BlockSpec(memory_space=pltpu.VMEM)
DMA = pltpu.SemaphoreType.DMA


def head_scratch():
    return [pltpu.VMEM((2 * ROWS, HALF), F32)] * 4 + [pltpu.VMEM((ROWS, HEAD), F32)] * 2


def local_call(pos, x, gains, freq, wq, wk, wv, wo, kc, vc):
    groups, n = ROWS // GROUP, kc.shape[1]
    table = pltpu.VMEM((ROWS, HALF), F32)
    return pl.pallas_call(
        local_kernel,
        name="local_attention",
        out_shape=(jax.ShapeDtypeStruct(kc.shape, BF16), jax.ShapeDtypeStruct(vc.shape, BF16),
                   pltpu.VMEM((2, ROWS, SIDE), BF16), table, table, pltpu.VMEM(x.shape, BF16)),
        in_specs=[ANY] * 10,
        out_specs=(IN_HBM, IN_HBM, IN_VMEM, IN_VMEM, IN_VMEM, IN_VMEM),
        scratch_shapes=[
            pltpu.SMEM((ROWS,), jnp.int32),
            pltpu.VMEM((4, D), F32), pltpu.VMEM((1, HALF), F32),
            pltpu.VMEM((D, 2 * HEAD), BF16), pltpu.VMEM((D, HEAD), BF16), pltpu.VMEM((D, HEAD), BF16), pltpu.VMEM((2 * HEAD, D), BF16),
            pltpu.VMEM((groups, GROUP, n, HEAD), BF16), pltpu.VMEM((groups, GROUP, n, HEAD), BF16),
        ] + head_scratch() + [DMA((4,)), DMA((4,))] + [DMA((groups,))] * 4,
        compiler_params=pltpu.CompilerParams(vmem_limit_bytes=40 * MIB),
    )(*[in_hbm(v) for v in (pos, x, gains, freq, wq, wk, wv, wo, kc, vc)])


def global_call(pos, a, cos_part, sin_part, ahead, kc, vc):
    groups, n = ROWS // GROUP, kc.shape[1]
    first = pltpu.VMEM((GROUP, n, HEAD), BF16)
    return pl.pallas_call(
        global_kernel,
        name="global_attention",
        out_shape=(jax.ShapeDtypeStruct(kc.shape, BF16), jax.ShapeDtypeStruct(vc.shape, BF16),
                   pltpu.VMEM((2, ROWS, SIDE), BF16), first, first),
        in_specs=[ANY] + [IN_VMEM] * 9 + [ANY] * 2,
        out_specs=(IN_HBM, IN_HBM, IN_VMEM, IN_VMEM, IN_VMEM),
        input_output_aliases={8: 3, 9: 4},
        scratch_shapes=[
            pltpu.SMEM((ROWS,), jnp.int32),
            pltpu.VMEM((groups - 1, GROUP, n, HEAD), BF16), pltpu.VMEM((groups - 1, GROUP, n, HEAD), BF16),
        ] + head_scratch() + [DMA(())] + [DMA((groups - 1,))] * 2 + [DMA((groups,))] * 2,
        compiler_params=pltpu.CompilerParams(vmem_limit_bytes=42 * MIB),
    )(in_hbm(pos), *[in_vmem(v) for v in (a, cos_part, sin_part, *ahead)], in_hbm(kc), in_hbm(vc))


def mlp_call(layer, x, o, gains, wg, wu, wd, ahead=()):
    square = pltpu.VMEM((D, D), BF16)
    full = pltpu.VMEM((ROWS, D), BF16)
    side = pltpu.VMEM((ROWS, SIDE), BF16)
    both = pltpu.VMEM((2, ROWS, SIDE), BF16)
    rows = pltpu.VMEM((ROWS, D), BF16)
    out_shape = [rows]
    if ahead:
        out_shape += [rows] + [pltpu.VMEM(w.shape[1:], BF16) for w in ahead[:4]]
        out_shape += [pltpu.VMEM((GROUP,) + c.shape[1:], BF16) for c in ahead[4:]]
    return pl.pallas_call(
        functools.partial(mlp_kernel, layer),
        name=f"mlp{layer}",
        out_shape=out_shape,
        in_specs=[IN_VMEM] * 2 + [ANY] * (4 + len(ahead)),
        out_specs=[IN_VMEM] * len(out_shape),
        scratch_shapes=[
            full, pltpu.VMEM((2, 4, D), F32), square, square, square, full,
            side, side, side, both, full, full, full, full, pltpu.VMEM((ROWS, D), F32),
            DMA(()), DMA((len(WIDE),)), DMA((len(WIDE),)), DMA((len(DOWN),)), DMA((6,)), DMA((3,)), DMA((3,)),
        ] + [DMA((len(DOWN),))] * 4,
        compiler_params=pltpu.CompilerParams(collective_id=layer, has_side_effects=True, vmem_limit_bytes=40 * MIB),
    )(in_vmem(x), in_vmem(o), *[in_hbm(v) for v in (gains, wg, wu, wd) + tuple(ahead)])


def decode_step(hidden, positions, k_local, v_local, k_global, v_global, w_query, w_key, w_value, w_out, w_gate, w_up, w_down, norm_scale):
    freq = jnp.asarray((ROPE_BASE ** (-2.0 * np.arange(HALF) / HEAD)).astype(np.float32).reshape(1, HALF))

    def flat(cache):
        return cache.reshape(cache.shape[0], cache.shape[1], HEAD)

    kg, vg = flat(k_global), flat(v_global)
    kl_new, vl_new, o, cos_part, sin_part, x = local_call(positions, hidden, norm_scale, freq, w_query, w_key, w_value, w_out, flat(k_local), flat(v_local))
    x, a, *ahead = mlp_call(0, x, o, norm_scale, w_gate, w_up, w_down, (w_query, w_key, w_value, w_out, kg, vg))
    kg_new, vg_new, o, _, _ = global_call(positions, a, cos_part, sin_part, ahead, kg, vg)
    (x,) = mlp_call(1, x, o, norm_scale, w_gate, w_up, w_down)
    return (x, kl_new.reshape(k_local.shape), vl_new.reshape(v_local.shape), kg_new.reshape(k_global.shape), vg_new.reshape(v_global.shape))


def solution(mesh):
    row_spec = P('dp', None)
    cache_spec = P('dp', None, 'tp', None)
    col_split = P(None, None, 'tp')
    row_split = P(None, 'tp', None)
    in_specs = (row_spec, P('dp'), cache_spec, cache_spec, cache_spec, cache_spec, col_split, col_split, col_split, row_split, col_split, col_split, row_split, P())
    out_specs = (row_spec, cache_spec, cache_spec, cache_spec, cache_spec)
    return jax.shard_map(decode_step, mesh=mesh, in_specs=in_specs, out_specs=out_specs, check_vma=False)
```

```python
import functools

import jax
import jax.numpy as jnp
import numpy as np
from jax import lax
from jax.experimental import pallas as pl
from jax.experimental.pallas import tpu as pltpu
from jax.sharding import PartitionSpec as P

SOFT_CAP = 50.0
NORM_EPS = 1e-6
ROPE_BASE = 10000.0
ROWS = 24
D = 2560
HEAD = 256
HALF = 128
GROUP = 4
CHUNK = 512
SIDE = D // 2
MIB = 2 ** 20
WRITES_FROM = 4
WIDE = ((0, 1536), (1536, 1024))
DOWN = ((0, 1280), (1280, 768), (2048, 512))
F32 = jnp.float32
BF16 = jnp.bfloat16


def normed(values, gain_row):
    inv_rms = lax.rsqrt(jnp.mean(values * values, axis=-1, keepdims=True) + NORM_EPS)
    return (values * inv_rms * (1.0 + gain_row)).astype(BF16)


def rotation(pos, freq):
    row_ids = lax.broadcasted_iota(jnp.int32, (ROWS, HALF), 0)
    pos_rows = jnp.zeros((ROWS, HALF), jnp.int32)
    for b in range(ROWS):
        pos_rows = jnp.where(row_ids == b, pos[b], pos_rows)
    angles = pos_rows.astype(F32) * freq
    return jnp.cos(angles), jnp.sin(angles)


def rotate(t, cos_part, sin_part):
    first, second = t[:, :HALF], t[:, HALF:]
    return first * cos_part - second * sin_part, second * cos_part + first * sin_part


def store_queries(q, cos_part, sin_part, qa, qb):
    for h in range(2):
        first, second = rotate(q[:, h * HEAD:(h + 1) * HEAD], cos_part, sin_part)
        qa[pl.ds(h, ROWS, stride=2), :] = first
        qb[pl.ds(h, ROWS, stride=2), :] = second


def store_key(k, cos_part, sin_part, knew):
    first, second = rotate(k, cos_part, sin_part)
    knew[:, :HALF] = first
    knew[:, HALF:] = second


def patch(buf, j, row, b, new):
    base = pl.multiple_of((row // 16) * 16, 16)
    tile = buf[j, pl.ds(base, 16), :].astype(F32)
    hit = lax.broadcasted_iota(jnp.int32, (16, HEAD), 0) == row - base
    fresh = jnp.broadcast_to(new[pl.ds(b, 1), :], (16, HEAD))
    buf[j, pl.ds(base, 16), :] = jnp.where(hit, fresh, tile).astype(BF16)


def attend_group(masked, g, pos, kref, vref, wait_k, wait_v, qa, qb, ma, mb, knew, vnew):
    n = kref.shape[1]
    rows8 = pl.ds(g * 8 if isinstance(g, int) else pl.multiple_of(g * 8, 8), 8)
    wait_k()
    for j in range(GROUP):
        b = g * GROUP + j
        patch(kref, j, lax.rem(pos[b], n), b, knew)
    q8 = jnp.concatenate([qa[rows8, :], qb[rows8, :]], axis=1).astype(BF16)
    owner = lax.broadcasted_iota(jnp.int32, (8, n), 0) // 2
    s = None
    for j in range(GROUP):
        part = lax.dot_general(q8, kref[j], (((1,), (1,)), ((), ())), preferred_element_type=F32)
        s = part if s is None else jnp.where(owner == j, part, s)
    e = jnp.exp(SOFT_CAP * jnp.tanh(s * (HEAD ** -0.5 / SOFT_CAP)))
    if masked:
        limit_rows = lax.broadcasted_iota(jnp.int32, (8, 1), 0) // 2
        limit = jnp.zeros((8, 1), jnp.int32)
        for j in range(GROUP):
            limit = jnp.where(limit_rows == j, pos[g * GROUP + j], limit)
        e = jnp.where(lax.broadcasted_iota(jnp.int32, (8, n), 1) <= limit, e, 0.0)
    p = (e / jnp.sum(e, axis=-1, keepdims=True)).astype(BF16)
    wait_v()
    for j in range(GROUP):
        b = g * GROUP + j
        patch(vref, j, lax.rem(pos[b], n), b, vnew)
    owner = lax.broadcasted_iota(jnp.int32, (8, HEAD), 0) // 2
    m = None
    for j in range(GROUP):
        part = jnp.dot(p, vref[j], preferred_element_type=F32)
        m = part if m is None else jnp.where(owner == j, part, m)
    ma[rows8, :] = m[:, :HALF]
    mb[rows8, :] = m[:, HALF:]


def project_out(ma, mb, wo, o_ref):
    mixed = jnp.concatenate([ref[pl.ds(h, ROWS, stride=2), :] for h in range(2) for ref in (ma, mb)], axis=1).astype(BF16)
    for c in range(2):
        o_ref[c] = jnp.dot(mixed, wo[:, c * SIDE:(c + 1) * SIDE], preferred_element_type=F32).astype(BF16)


def group_rows(ref, g):
    return ref.at[pl.ds(g * GROUP, GROUP)]


def local_kernel(pos_hbm, x_hbm, gain_hbm, freq_hbm, wq_hbm, wk_hbm, wv_hbm, wo_hbm, kc_hbm, vc_hbm,
                 ko_hbm, vo_hbm, o_ref, cos_ref, sin_ref, x,
                 pos, gain, freq, wq, wk, wv, wo, kbuf, vbuf, qa, qb, ma, mb, knew, vnew,
                 small_sem, w_sem, kr_sem, vr_sem, kw_sem, vw_sem):
    groups = ROWS // GROUP
    small = [pltpu.make_async_copy(s, d, small_sem.at[i]) for i, (s, d) in enumerate(
        ((x_hbm, x), (gain_hbm.at[0], gain), (pos_hbm, pos), (freq_hbm, freq)))]
    weights = [pltpu.make_async_copy(s.at[0], d, w_sem.at[i]) for i, (s, d) in enumerate(
        ((wq_hbm, wq), (wk_hbm, wk), (wv_hbm, wv), (wo_hbm, wo)))]

    def k_read(g):
        return pltpu.make_async_copy(group_rows(kc_hbm, g), kbuf.at[g], kr_sem.at[g])

    def v_read(g):
        return pltpu.make_async_copy(group_rows(vc_hbm, g), vbuf.at[g], vr_sem.at[g])

    def writes(g):
        return (pltpu.make_async_copy(kbuf.at[g], group_rows(ko_hbm, g), kw_sem.at[g]),
                pltpu.make_async_copy(vbuf.at[g], group_rows(vo_hbm, g), vw_sem.at[g]))

    for copy in small:
        copy.start()
    for copy in weights[:3]:
        copy.start(priority=1)
    for g in range(groups):
        k_read(g).start(priority=1)
        v_read(g).start(priority=1)
    weights[3].start(priority=1)

    for copy in small:
        copy.wait()
    cos_part, sin_part = rotation(pos, freq[...])
    cos_ref[...] = cos_part
    sin_ref[...] = sin_part
    a = normed(x[...].astype(F32), gain[0:1, :])
    weights[0].wait()
    store_queries(jnp.dot(a, wq[...], preferred_element_type=F32), cos_part, sin_part, qa, qb)
    weights[1].wait()
    store_key(jnp.dot(a, wk[...], preferred_element_type=F32), cos_part, sin_part, knew)
    weights[2].wait()
    vnew[...] = jnp.dot(a, wv[...], preferred_element_type=F32)

    def step(g, carry):
        attend_group(False, g, pos, kbuf.at[g], vbuf.at[g], lambda: k_read(g).wait(), lambda: v_read(g).wait(), qa, qb, ma, mb, knew, vnew)
        for copy in writes(g):
            copy.start(priority=1)
        return carry

    lax.fori_loop(0, groups, step, 0)
    weights[3].wait()
    project_out(ma, mb, wo, o_ref)
    for g in range(groups):
        for copy in writes(g):
            copy.wait()


def global_kernel(pos_hbm, a_ref, cos_ref, sin_ref, wq, wk, wv, wo, _k_first, _v_first, kc_hbm, vc_hbm,
                  ko_hbm, vo_hbm, o_ref, kfirst, vfirst,
                  pos, kbuf, vbuf, qa, qb, ma, mb, knew, vnew,
                  pos_sem, kr_sem, vr_sem, kw_sem, vw_sem):
    groups = ROWS // GROUP
    pos_copy = pltpu.make_async_copy(pos_hbm, pos, pos_sem)

    def k_read(g):
        return pltpu.make_async_copy(group_rows(kc_hbm, g), kbuf.at[g - 1], kr_sem.at[g - 1])

    def v_read(g):
        return pltpu.make_async_copy(group_rows(vc_hbm, g), vbuf.at[g - 1], vr_sem.at[g - 1])

    def writes(g, k, v):
        return (pltpu.make_async_copy(k, group_rows(ko_hbm, g), kw_sem.at[g]),
                pltpu.make_async_copy(v, group_rows(vo_hbm, g), vw_sem.at[g]))

    def start_writes(g):
        for copy in writes(g, kfirst if g == 0 else kbuf.at[g - 1], vfirst if g == 0 else vbuf.at[g - 1]):
            copy.start(priority=1)

    pos_copy.start()
    for g in range(1, groups):
        k_read(g).start(priority=1)
        v_read(g).start(priority=1)
    cos_part, sin_part = cos_ref[...], sin_ref[...]
    a = a_ref[...]
    store_queries(jnp.dot(a, wq[...], preferred_element_type=F32), cos_part, sin_part, qa, qb)
    store_key(jnp.dot(a, wk[...], preferred_element_type=F32), cos_part, sin_part, knew)
    vnew[...] = jnp.dot(a, wv[...], preferred_element_type=F32)
    pos_copy.wait()

    attend_group(True, 0, pos, kfirst, vfirst, lambda: None, lambda: None, qa, qb, ma, mb, knew, vnew)

    def step(g, carry):
        k, v = kbuf.at[g - 1], vbuf.at[g - 1]

        def wait_v():
            v_read(g).wait()

            @pl.when(g == WRITES_FROM)
            def _():
                for i in range(WRITES_FROM):
                    start_writes(i)

        attend_group(True, g, pos, k, v, lambda: k_read(g).wait(), wait_v, qa, qb, ma, mb, knew, vnew)

        @pl.when(g >= WRITES_FROM)
        def _():
            for copy in writes(g, k, v):
                copy.start(priority=1)
        return carry

    lax.fori_loop(1, groups, step, 0)
    project_out(ma, mb, wo, o_ref)
    for copy in writes(0, kfirst, vfirst):
        copy.wait()
    for g in range(1, groups):
        for copy in writes(g, kbuf.at[g - 1], vbuf.at[g - 1]):
            copy.wait()


def mlp_kernel(layer, *refs):
    n_in, n_out = (12, 8) if layer == 0 else (6, 1)
    x_ref, o_ref, gain_hbm, wg_hbm, wu_hbm, wd_hbm = refs[:6]
    outs = refs[n_in:n_in + n_out]
    (x, gain, wg, wu, wd, h, ohalf, orecv1, orecv2, osum, fsend, fhalf, frecv1, frecv2, total,
     small_sem, g_sem, u_sem, d_sem, ahead_sem, o_send, o_recv, fs1, fr1, fs2, fr2) = refs[n_in + n_out:]
    out_ref = outs[0]
    last = len(DOWN)
    me = lax.axis_index("tp")
    chip, core = me // 2, lax.rem(me, 2)
    partner = chip * 2 + (1 - core)
    across = (1 - chip) * 2 + (1 - core)
    side = lax.rem(chip + core, 2)

    gain_copy = pltpu.make_async_copy(gain_hbm, gain, small_sem)
    wide_cols = [pl.ds(start, size) for start, size in WIDE]
    down_cols = [pl.ds(start, size) for start, size in DOWN]
    gates = [pltpu.make_async_copy(wg_hbm.at[layer, :, d], wg.at[:, d], g_sem.at[i]) for i, d in enumerate(wide_cols)]
    ups = [pltpu.make_async_copy(wu_hbm.at[layer, :, d], wu.at[:, d], u_sem.at[i]) for i, d in enumerate(wide_cols)]
    downs = [pltpu.make_async_copy(wd_hbm.at[layer, :, d], wd.at[:, d], d_sem.at[i]) for i, d in enumerate(down_cols)]
    ahead = []
    if layer == 0:
        wq_hbm, wk_hbm, wv_hbm, wo_hbm, kc_hbm, vc_hbm = refs[6:12]
        sources = [w.at[1] for w in (wq_hbm, wk_hbm, wv_hbm, wo_hbm)] + [group_rows(kc_hbm, 0), group_rows(vc_hbm, 0)]
        ahead = [pltpu.make_async_copy(s, d, ahead_sem.at[i]) for i, (s, d) in enumerate(zip(sources, outs[2:]))]

    def start_bulk(copies):
        for copy in copies:
            copy.start(priority=1)

    gain_copy.start()
    start_bulk((gates[0], ups[0]))

    barrier = pltpu.get_barrier_semaphore()
    for peer in (partner, across):
        pl.semaphore_signal(barrier, inc=1, device_id={"tp": peer}, device_id_type=pl.DeviceIdType.MESH)
    pl.semaphore_wait(barrier, 2)

    def remote(src, dst, send, recv, peer):
        return pltpu.make_async_remote_copy(src_ref=src, dst_ref=dst, send_sem=send, recv_sem=recv,
                                            device_id={"tp": peer}, device_id_type=pl.DeviceIdType.MESH)

    o_copies = (remote(o_ref.at[1 - side], orecv1, o_send.at[0], o_recv.at[0], partner),
                remote(ohalf, orecv2, o_send.at[1], o_recv.at[1], across),
                remote(osum.at[side], osum.at[side], o_send.at[2], o_recv.at[2], partner))
    o_copies[0].start()
    start_bulk((gates[1], ups[1]))
    gain_copy.wait()
    o_copies[0].wait_recv()
    ohalf[...] = (o_ref[side].astype(F32) + orecv1[...].astype(F32)).astype(BF16)
    o_copies[1].start()
    o_copies[1].wait_recv()
    osum[side] = (ohalf[...].astype(F32) + orecv2[...].astype(F32)).astype(BF16)
    o_copies[2].start()
    o_copies[2].wait_recv()
    o_sum = jnp.concatenate([osum[0], osum[1]], axis=1).astype(F32)
    x1 = (x_ref[...].astype(F32) + normed(o_sum, gain[layer, 1:2, :]).astype(F32)).astype(BF16)
    x[...] = x1
    a = normed(x1.astype(F32), gain[layer, 2:3, :])

    for w, (start, size) in enumerate(WIDE):
        gates[w].wait()
        ups[w].wait()
        start_bulk(downs if w == 0 else ahead)
        for c in range(start, start + size, CHUNK):
            gate = jnp.dot(a, wg[:, c:c + CHUNK], preferred_element_type=F32)
            up = jnp.dot(a, wu[:, c:c + CHUNK], preferred_element_type=F32)
            h[:, c:c + CHUNK] = (jax.nn.gelu(gate, approximate=True) * up).astype(BF16)
    act = h[...]

    def to_partner(c):
        d = down_cols[c]
        return remote(fsend.at[:, d], frecv1.at[:, d], fs1.at[c], fr1.at[c], partner)

    def to_across(c):
        d = down_cols[c]
        return remote(fhalf.at[:, d], frecv2.at[:, d], fs2.at[c], fr2.at[c], across)

    def relay(c):
        d = down_cols[c]
        to_partner(c).wait_recv()
        fhalf[:, d] = (fsend[:, d].astype(F32) + frecv1[:, d].astype(F32)).astype(BF16)
        to_across(c).start()

    for c in range(last):
        downs[c].wait()
        fsend[:, down_cols[c]] = jnp.dot(act, wd[:, down_cols[c]], preferred_element_type=F32).astype(BF16)
        to_partner(c).start()
        if c >= 1:
            relay(c - 1)
    for c in range(last - 1, last):
        relay(c)
    squares = jnp.zeros((ROWS, HALF), F32)
    for c in range(last):
        to_across(c).wait_recv()
        piece = fhalf[:, down_cols[c]].astype(F32) + frecv2[:, down_cols[c]].astype(F32)
        total[:, down_cols[c]] = piece
        for i in range(DOWN[c][1] // HALF):
            lane_block = piece[:, i * HALF:(i + 1) * HALF]
            squares = squares + lane_block * lane_block
    inv_rms = lax.rsqrt(jnp.sum(squares, axis=-1, keepdims=True) / D + NORM_EPS)
    branch = (total[...] * inv_rms * (1.0 + gain[layer, 3:4, :])).astype(BF16)
    x2 = (x[...].astype(F32) + branch.astype(F32)).astype(BF16)
    out_ref[...] = x2
    if layer == 0:
        outs[1][...] = normed(x2.astype(F32), gain[1, 0:1, :])
    for copy in o_copies:
        copy.wait_send()
    for c in range(last):
        to_partner(c).wait_send()
        to_across(c).wait_send()
    for copy in ahead:
        copy.wait()


def in_hbm(value):
    return pltpu.with_memory_space_constraint(value, pltpu.HBM)


def in_vmem(value):
    return pltpu.with_memory_space_constraint(value, pltpu.VMEM)


ANY = pl.BlockSpec(memory_space=pl.ANY)
IN_HBM = pl.BlockSpec(memory_space=pltpu.HBM)
IN_VMEM = pl.BlockSpec(memory_space=pltpu.VMEM)
DMA = pltpu.SemaphoreType.DMA


def head_scratch():
    return [pltpu.VMEM((2 * ROWS, HALF), F32)] * 4 + [pltpu.VMEM((ROWS, HEAD), F32)] * 2


def local_call(pos, x, gains, freq, wq, wk, wv, wo, kc, vc):
    groups, n = ROWS // GROUP, kc.shape[1]
    table = pltpu.VMEM((ROWS, HALF), F32)
    return pl.pallas_call(
        local_kernel,
        name="local_attention",
        out_shape=(jax.ShapeDtypeStruct(kc.shape, BF16), jax.ShapeDtypeStruct(vc.shape, BF16),
                   pltpu.VMEM((2, ROWS, SIDE), BF16), table, table, pltpu.VMEM(x.shape, BF16)),
        in_specs=[ANY] * 10,
        out_specs=(IN_HBM, IN_HBM, IN_VMEM, IN_VMEM, IN_VMEM, IN_VMEM),
        scratch_shapes=[
            pltpu.SMEM((ROWS,), jnp.int32),
            pltpu.VMEM((4, D), F32), pltpu.VMEM((1, HALF), F32),
            pltpu.VMEM((D, 2 * HEAD), BF16), pltpu.VMEM((D, HEAD), BF16), pltpu.VMEM((D, HEAD), BF16), pltpu.VMEM((2 * HEAD, D), BF16),
            pltpu.VMEM((groups, GROUP, n, HEAD), BF16), pltpu.VMEM((groups, GROUP, n, HEAD), BF16),
        ] + head_scratch() + [DMA((4,)), DMA((4,))] + [DMA((groups,))] * 4,
        compiler_params=pltpu.CompilerParams(vmem_limit_bytes=40 * MIB),
    )(*[in_hbm(v) for v in (pos, x, gains, freq, wq, wk, wv, wo, kc, vc)])


def global_call(pos, a, cos_part, sin_part, ahead, kc, vc):
    groups, n = ROWS // GROUP, kc.shape[1]
    first = pltpu.VMEM((GROUP, n, HEAD), BF16)
    return pl.pallas_call(
        global_kernel,
        name="global_attention",
        out_shape=(jax.ShapeDtypeStruct(kc.shape, BF16), jax.ShapeDtypeStruct(vc.shape, BF16),
                   pltpu.VMEM((2, ROWS, SIDE), BF16), first, first),
        in_specs=[ANY] + [IN_VMEM] * 9 + [ANY] * 2,
        out_specs=(IN_HBM, IN_HBM, IN_VMEM, IN_VMEM, IN_VMEM),
        input_output_aliases={8: 3, 9: 4},
        scratch_shapes=[
            pltpu.SMEM((ROWS,), jnp.int32),
            pltpu.VMEM((groups - 1, GROUP, n, HEAD), BF16), pltpu.VMEM((groups - 1, GROUP, n, HEAD), BF16),
        ] + head_scratch() + [DMA(())] + [DMA((groups - 1,))] * 2 + [DMA((groups,))] * 2,
        compiler_params=pltpu.CompilerParams(vmem_limit_bytes=42 * MIB),
    )(in_hbm(pos), *[in_vmem(v) for v in (a, cos_part, sin_part, *ahead)], in_hbm(kc), in_hbm(vc))


def mlp_call(layer, x, o, gains, wg, wu, wd, ahead=()):
    square = pltpu.VMEM((D, D), BF16)
    full = pltpu.VMEM((ROWS, D), BF16)
    side = pltpu.VMEM((ROWS, SIDE), BF16)
    both = pltpu.VMEM((2, ROWS, SIDE), BF16)
    rows = pltpu.VMEM((ROWS, D), BF16)
    out_shape = [rows]
    if ahead:
        out_shape += [rows] + [pltpu.VMEM(w.shape[1:], BF16) for w in ahead[:4]]
        out_shape += [pltpu.VMEM((GROUP,) + c.shape[1:], BF16) for c in ahead[4:]]
    return pl.pallas_call(
        functools.partial(mlp_kernel, layer),
        name=f"mlp{layer}",
        out_shape=out_shape,
        in_specs=[IN_VMEM] * 2 + [ANY] * (4 + len(ahead)),
        out_specs=[IN_VMEM] * len(out_shape),
        scratch_shapes=[
            full, pltpu.VMEM((2, 4, D), F32), square, square, square, full,
            side, side, side, both, full, full, full, full, pltpu.VMEM((ROWS, D), F32),
            DMA(()), DMA((len(WIDE),)), DMA((len(WIDE),)), DMA((len(DOWN),)), DMA((6,)), DMA((3,)), DMA((3,)),
        ] + [DMA((len(DOWN),))] * 4,
        compiler_params=pltpu.CompilerParams(collective_id=layer, has_side_effects=True, vmem_limit_bytes=40 * MIB),
    )(in_vmem(x), in_vmem(o), *[in_hbm(v) for v in (gains, wg, wu, wd) + tuple(ahead)])


def decode_step(hidden, positions, k_local, v_local, k_global, v_global, w_query, w_key, w_value, w_out, w_gate, w_up, w_down, norm_scale):
    freq = jnp.asarray((ROPE_BASE ** (-2.0 * np.arange(HALF) / HEAD)).astype(np.float32).reshape(1, HALF))

    def flat(cache):
        return cache.reshape(cache.shape[0], cache.shape[1], HEAD)

    kg, vg = flat(k_global), flat(v_global)
    kl_new, vl_new, o, cos_part, sin_part, x = local_call(positions, hidden, norm_scale, freq, w_query, w_key, w_value, w_out, flat(k_local), flat(v_local))
    x, a, *ahead = mlp_call(0, x, o, norm_scale, w_gate, w_up, w_down, (w_query, w_key, w_value, w_out, kg, vg))
    kg_new, vg_new, o, _, _ = global_call(positions, a, cos_part, sin_part, ahead, kg, vg)
    (x,) = mlp_call(1, x, o, norm_scale, w_gate, w_up, w_down)
    return (x, kl_new.reshape(k_local.shape), vl_new.reshape(v_local.shape), kg_new.reshape(k_global.shape), vg_new.reshape(v_global.shape))


def solution(mesh):
    row_spec = P('dp', None)
    cache_spec = P('dp', None, 'tp', None)
    col_split = P(None, None, 'tp')
    row_split = P(None, 'tp', None)
    in_specs = (row_spec, P('dp'), cache_spec, cache_spec, cache_spec, cache_spec, col_split, col_split, col_split, row_split, col_split, col_split, row_split, P())
    out_specs = (row_spec, cache_spec, cache_spec, cache_spec, cache_spec)
    return jax.shard_map(decode_step, mesh=mesh, in_specs=in_specs, out_specs=out_specs, check_vma=False)
```

```python
import functools

import jax
import jax.numpy as jnp
import numpy as np
from jax import lax
from jax.experimental import pallas as pl
from jax.experimental.pallas import tpu as pltpu
from jax.sharding import PartitionSpec as P

SOFT_CAP = 50.0
NORM_EPS = 1e-6
ROPE_BASE = 10000.0
ROWS = 24
D = 2560
HEAD = 256
HALF = 128
GROUP = 4
CHUNK = 512
SIDE = D // 2
MIB = 2 ** 20
FIRST = 3
FF_PART = D // 2
PIECE = 256
F32 = jnp.float32
BF16 = jnp.bfloat16


def normed(values, gain_row):
    inv_rms = lax.rsqrt(jnp.mean(values * values, axis=-1, keepdims=True) + NORM_EPS)
    return (values * inv_rms * (1.0 + gain_row)).astype(BF16)


def rotation(pos, freq):
    row_ids = lax.broadcasted_iota(jnp.int32, (ROWS, HALF), 0)
    pos_rows = jnp.zeros((ROWS, HALF), jnp.int32)
    for b in range(ROWS):
        pos_rows = jnp.where(row_ids == b, pos[b], pos_rows)
    angles = pos_rows.astype(F32) * freq
    return jnp.cos(angles), jnp.sin(angles)


def rotate(t, cos_part, sin_part):
    first, second = t[:, :HALF], t[:, HALF:]
    return first * cos_part - second * sin_part, second * cos_part + first * sin_part


def store_queries(q, cos_part, sin_part, qa, qb):
    for h in range(2):
        first, second = rotate(q[:, h * HEAD:(h + 1) * HEAD], cos_part, sin_part)
        qa[pl.ds(h, ROWS, stride=2), :] = first
        qb[pl.ds(h, ROWS, stride=2), :] = second


def store_key(k, cos_part, sin_part, knew):
    first, second = rotate(k, cos_part, sin_part)
    knew[:, :HALF] = first
    knew[:, HALF:] = second


def patch(buf, j, row, b, new):
    base = pl.multiple_of((row // 16) * 16, 16)
    tile = buf[j, pl.ds(base, 16), :].astype(F32)
    hit = lax.broadcasted_iota(jnp.int32, (16, HEAD), 0) == row - base
    fresh = jnp.broadcast_to(new[pl.ds(b, 1), :], (16, HEAD))
    buf[j, pl.ds(base, 16), :] = jnp.where(hit, fresh, tile).astype(BF16)


def attend_group(masked, g, pos, kref, vref, wait_k, wait_v, qa, qb, ma, mb, knew, vnew):
    n = kref.shape[1]
    rows8 = pl.ds(g * 8 if isinstance(g, int) else pl.multiple_of(g * 8, 8), 8)
    wait_k()
    for j in range(GROUP):
        b = g * GROUP + j
        patch(kref, j, lax.rem(pos[b], n), b, knew)
    q8 = jnp.concatenate([qa[rows8, :], qb[rows8, :]], axis=1).astype(BF16)
    owner = lax.broadcasted_iota(jnp.int32, (8, n), 0) // 2
    s = None
    for j in range(GROUP):
        part = lax.dot_general(q8, kref[j], (((1,), (1,)), ((), ())), preferred_element_type=F32)
        s = part if s is None else jnp.where(owner == j, part, s)
    e = jnp.exp(SOFT_CAP * jnp.tanh(s * (HEAD ** -0.5 / SOFT_CAP)))
    if masked:
        limit_rows = lax.broadcasted_iota(jnp.int32, (8, 1), 0) // 2
        limit = jnp.zeros((8, 1), jnp.int32)
        for j in range(GROUP):
            limit = jnp.where(limit_rows == j, pos[g * GROUP + j], limit)
        e = jnp.where(lax.broadcasted_iota(jnp.int32, (8, n), 1) <= limit, e, 0.0)
    p = (e / jnp.sum(e, axis=-1, keepdims=True)).astype(BF16)
    wait_v()
    for j in range(GROUP):
        b = g * GROUP + j
        patch(vref, j, lax.rem(pos[b], n), b, vnew)
    owner = lax.broadcasted_iota(jnp.int32, (8, HEAD), 0) // 2
    m = None
    for j in range(GROUP):
        part = jnp.dot(p, vref[j], preferred_element_type=F32)
        m = part if m is None else jnp.where(owner == j, part, m)
    ma[rows8, :] = m[:, :HALF]
    mb[rows8, :] = m[:, HALF:]


def project_out(ma, mb, wo, o_ref):
    mixed = jnp.concatenate([ref[pl.ds(h, ROWS, stride=2), :] for h in range(2) for ref in (ma, mb)], axis=1).astype(BF16)
    for c in range(2):
        o_ref[c] = jnp.dot(mixed, wo[:, c * SIDE:(c + 1) * SIDE], preferred_element_type=F32).astype(BF16)


def group_rows(ref, g):
    return ref.at[pl.ds(g * GROUP, GROUP)]


def local_kernel(pos_hbm, x_hbm, gain_hbm, freq_hbm, wq_hbm, wk_hbm, wv_hbm, wo_hbm, kc_hbm, vc_hbm,
                 ko_hbm, vo_hbm, o_ref, cos_ref, sin_ref, x,
                 pos, gain, freq, wq, wk, wv, wo, kbuf, vbuf, qa, qb, ma, mb, knew, vnew,
                 small_sem, w_sem, kr_sem, vr_sem, kw_sem, vw_sem):
    groups = ROWS // GROUP
    small = [pltpu.make_async_copy(s, d, small_sem.at[i]) for i, (s, d) in enumerate(
        ((x_hbm, x), (gain_hbm.at[0], gain), (pos_hbm, pos), (freq_hbm, freq)))]
    weights = [pltpu.make_async_copy(s.at[0], d, w_sem.at[i]) for i, (s, d) in enumerate(
        ((wq_hbm, wq), (wk_hbm, wk), (wv_hbm, wv), (wo_hbm, wo)))]

    def k_read(g):
        return pltpu.make_async_copy(group_rows(kc_hbm, g), kbuf.at[g], kr_sem.at[g])

    def v_read(g):
        return pltpu.make_async_copy(group_rows(vc_hbm, g), vbuf.at[g], vr_sem.at[g])

    def writes(g):
        return (pltpu.make_async_copy(kbuf.at[g], group_rows(ko_hbm, g), kw_sem.at[g]),
                pltpu.make_async_copy(vbuf.at[g], group_rows(vo_hbm, g), vw_sem.at[g]))

    for copy in small:
        copy.start()
    for copy in weights[:3]:
        copy.start(priority=1)
    for g in range(groups):
        k_read(g).start(priority=1)
        v_read(g).start(priority=1)
    weights[3].start(priority=1)

    for copy in small:
        copy.wait()
    cos_part, sin_part = rotation(pos, freq[...])
    cos_ref[...] = cos_part
    sin_ref[...] = sin_part
    a = normed(x[...].astype(F32), gain[0:1, :])
    weights[0].wait()
    store_queries(jnp.dot(a, wq[...], preferred_element_type=F32), cos_part, sin_part, qa, qb)
    weights[1].wait()
    store_key(jnp.dot(a, wk[...], preferred_element_type=F32), cos_part, sin_part, knew)
    weights[2].wait()
    vnew[...] = jnp.dot(a, wv[...], preferred_element_type=F32)

    def step(g, carry):
        attend_group(False, g, pos, kbuf.at[g], vbuf.at[g], lambda: k_read(g).wait(), lambda: v_read(g).wait(), qa, qb, ma, mb, knew, vnew)
        for copy in writes(g):
            copy.start(priority=1)
        return carry

    lax.fori_loop(0, groups, step, 0)
    weights[3].wait()
    project_out(ma, mb, wo, o_ref)
    for g in range(groups):
        for copy in writes(g):
            copy.wait()


def global_kernel(pos_hbm, a_ref, cos_ref, sin_ref, wq, wk, wv, wo, *refs):
    kc_hbm, vc_hbm, ko_hbm, vo_hbm, o_ref = refs[2 * FIRST:2 * FIRST + 5]
    kfirst, vfirst = refs[2 * FIRST + 5:3 * FIRST + 5], refs[3 * FIRST + 5:4 * FIRST + 5]
    pos, kbuf, vbuf, qa, qb, ma, mb, knew, vnew, pos_sem, kr_sem, vr_sem, kw_sem, vw_sem = refs[4 * FIRST + 5:]
    groups = ROWS // GROUP
    pos_copy = pltpu.make_async_copy(pos_hbm, pos, pos_sem)

    def k_read(g):
        return pltpu.make_async_copy(group_rows(kc_hbm, g), kbuf.at[g - FIRST], kr_sem.at[g - FIRST])

    def v_read(g):
        return pltpu.make_async_copy(group_rows(vc_hbm, g), vbuf.at[g - FIRST], vr_sem.at[g - FIRST])

    def writes(g, k, v):
        return (pltpu.make_async_copy(k, group_rows(ko_hbm, g), kw_sem.at[g]),
                pltpu.make_async_copy(v, group_rows(vo_hbm, g), vw_sem.at[g]))

    pos_copy.start()
    for g in range(FIRST, groups):
        k_read(g).start(priority=1)
        v_read(g).start(priority=1)
    cos_part, sin_part = cos_ref[...], sin_ref[...]
    a = a_ref[...]
    store_queries(jnp.dot(a, wq[...], preferred_element_type=F32), cos_part, sin_part, qa, qb)
    store_key(jnp.dot(a, wk[...], preferred_element_type=F32), cos_part, sin_part, knew)
    vnew[...] = jnp.dot(a, wv[...], preferred_element_type=F32)
    pos_copy.wait()

    for g in range(FIRST):
        attend_group(True, g, pos, kfirst[g], vfirst[g], lambda: None, lambda: None, qa, qb, ma, mb, knew, vnew)
    for g in range(FIRST):
        for copy in writes(g, kfirst[g], vfirst[g]):
            copy.start(priority=1)

    def step(g, carry):
        k, v = kbuf.at[g - FIRST], vbuf.at[g - FIRST]
        attend_group(True, g, pos, k, v, lambda: k_read(g).wait(), lambda: v_read(g).wait(), qa, qb, ma, mb, knew, vnew)
        for copy in writes(g, k, v):
            copy.start(priority=1)
        return carry

    lax.fori_loop(FIRST, groups, step, 0)
    project_out(ma, mb, wo, o_ref)
    for g in range(groups):
        k, v = (kfirst[g], vfirst[g]) if g < FIRST else (kbuf.at[g - FIRST], vbuf.at[g - FIRST])
        for copy in writes(g, k, v):
            copy.wait()


def mlp_kernel(layer, *refs):
    n_in, n_out = (12, 6 + 2 * FIRST) if layer == 0 else (6, 1)
    x_ref, o_ref, gain_hbm, wg_hbm, wu_hbm, wd_hbm = refs[:6]
    outs = refs[n_in:n_in + n_out]
    (x, gain, wg, wu, wd, a48, h, x_other, opart, ohalf, ox, oy, oz, osum, fpart, fpair, fhalf, fx, fy, fz, fsum,
     small_sem, w_sem, ahead_sem, o_send, o_recv, x_send, x_recv, f_send, f_recv) = refs[n_in + n_out:]
    out_ref = outs[0]
    dp, me = lax.axis_index("dp"), lax.axis_index("tp")
    chip, core = me // 2, lax.rem(me, 2)
    side = lax.rem(chip + core, 2)
    partner = {"dp": dp, "tp": chip * 2 + (1 - core)}
    along = {"dp": dp, "tp": (1 - chip) * 2 + (1 - core)}
    beside = {"dp": 1 - dp, "tp": chip * 2 + core}
    opposite = {"dp": 1 - dp, "tp": (1 - chip) * 2 + (1 - core)}

    part = pl.ds(pl.multiple_of(dp * FF_PART, FF_PART), FF_PART)
    weights = [pltpu.make_async_copy(s, d, w_sem.at[i]) for i, (s, d) in enumerate(
        ((wg_hbm.at[layer, :, part], wg), (wu_hbm.at[layer, :, part], wu), (wd_hbm.at[layer, part, :], wd)))]
    gain_copy = pltpu.make_async_copy(gain_hbm, gain, small_sem)
    ahead = []
    if layer == 0:
        wq_hbm, wk_hbm, wv_hbm, wo_hbm, kc_hbm, vc_hbm = refs[6:12]
        pairs = list(zip([w.at[1] for w in (wq_hbm, wk_hbm, wv_hbm, wo_hbm)], outs[2:6]))
        for g in range(FIRST):
            pairs += [(group_rows(kc_hbm, g), outs[6 + g]), (group_rows(vc_hbm, g), outs[6 + FIRST + g])]
        ahead = [pltpu.make_async_copy(s, d, ahead_sem.at[i]) for i, (s, d) in enumerate(pairs)]

    gain_copy.start()
    for copy in weights:
        copy.start(priority=1)

    barrier = pltpu.get_barrier_semaphore()
    for peer in (partner, along, beside, opposite):
        pl.semaphore_signal(barrier, inc=1, device_id=peer, device_id_type=pl.DeviceIdType.MESH)
    pl.semaphore_wait(barrier, 4)

    def remote(src, dst, send, recv, peer):
        return pltpu.make_async_remote_copy(src_ref=src, dst_ref=dst, send_sem=send, recv_sem=recv,
                                            device_id=peer, device_id_type=pl.DeviceIdType.MESH)

    mine = pl.ds(pl.multiple_of(side * SIDE, SIDE), SIDE)
    theirs = pl.ds(pl.multiple_of((1 - side) * SIDE, SIDE), SIDE)

    o_copies = [remote(src, dst, o_send.at[i], o_recv.at[i], peer) for i, (src, dst, peer) in enumerate((
        (o_ref.at[1 - side], opart, partner), (ohalf, oz, opposite), (ohalf, oy, beside), (ohalf, ox, along),
        (osum.at[side], osum.at[side], partner)))]
    x_copies = [remote(src, dst, x_send.at[i], x_recv.at[i], peer) for i, (src, dst, peer) in enumerate((
        (x_ref.at[:, mine], x_other.at[:, mine], beside), (x_other.at[:, mine], x_other.at[:, mine], partner)))]
    o_copies[0].start()
    x_copies[0].start()
    for copy in ahead:
        copy.start(priority=1)
    gain_copy.wait()
    o_copies[0].wait_recv()
    ohalf[...] = (o_ref[side].astype(F32) + opart[...].astype(F32)).astype(BF16)
    for copy in o_copies[1:4]:
        copy.start()
    x_copies[0].wait_recv()
    x_copies[1].start()
    for copy in o_copies[1:4]:
        copy.wait_recv()
    osum[side, 0] = (ohalf[...].astype(F32) + ox[...].astype(F32)).astype(BF16)
    osum[side, 1] = (oy[...].astype(F32) + oz[...].astype(F32)).astype(BF16)
    o_copies[4].start()
    x_copies[1].wait_recv()
    o_copies[4].wait_recv()
    for group, rows in enumerate((x_ref, x_other)):
        o_rows = jnp.concatenate([osum[0, group], osum[1, group]], axis=1).astype(F32)
        x1 = (rows[...].astype(F32) + normed(o_rows, gain[layer, 1:2, :]).astype(F32)).astype(BF16)
        if group == 0:
            x[...] = x1
        a48[group * ROWS:(group + 1) * ROWS, :] = normed(x1.astype(F32), gain[layer, 2:3, :])
    weights[0].wait()
    weights[1].wait()
    a = a48[...]
    for c in range(0, FF_PART, PIECE):
        gate = jnp.dot(a, wg[:, c:c + PIECE], preferred_element_type=F32)
        up = jnp.dot(a, wu[:, c:c + PIECE], preferred_element_type=F32)
        h[:, c:c + PIECE] = (jax.nn.gelu(gate, approximate=True) * up).astype(BF16)
    weights[2].wait()
    act = h[...]

    f_copies = [remote(src, dst, f_send.at[i], f_recv.at[i], peer) for i, (src, dst, peer) in enumerate((
        (fpart.at[1 - side], fpair, partner), (fhalf.at[1], fz, opposite), (fhalf.at[1], fy, beside), (fhalf.at[0], fx, along),
        (fsum.at[side], fsum.at[side], partner)))]
    for which, columns in ((1 - side, theirs), (side, mine)):
        partial = jnp.dot(act, wd[:, columns], preferred_element_type=F32)
        fpart[which, 0] = partial[:ROWS].astype(BF16)
        fpart[which, 1] = partial[ROWS:].astype(BF16)
        if which is not side:
            f_copies[0].start()
    f_copies[0].wait_recv()
    for group in (1, 0):
        fhalf[group] = (fpart[side, group].astype(F32) + fpair[group].astype(F32)).astype(BF16)
    for copy in f_copies[1:4]:
        copy.start()
    for copy in f_copies[1:4]:
        copy.wait_recv()
    fsum[side] = ((fhalf[0].astype(F32) + fx[...].astype(F32)) + (fy[...].astype(F32) + fz[...].astype(F32))).astype(BF16)
    f_copies[4].start()
    f_copies[4].wait_recv()
    f_rows = jnp.concatenate([fsum[0], fsum[1]], axis=1).astype(F32)
    x2 = (x[...].astype(F32) + normed(f_rows, gain[layer, 3:4, :]).astype(F32)).astype(BF16)
    out_ref[...] = x2
    if layer == 0:
        outs[1][...] = normed(x2.astype(F32), gain[1, 0:1, :])
    for copy in o_copies + x_copies + f_copies:
        copy.wait_send()
    for copy in ahead:
        copy.wait()


def in_hbm(value):
    return pltpu.with_memory_space_constraint(value, pltpu.HBM)


def in_vmem(value):
    return pltpu.with_memory_space_constraint(value, pltpu.VMEM)


ANY = pl.BlockSpec(memory_space=pl.ANY)
IN_HBM = pl.BlockSpec(memory_space=pltpu.HBM)
IN_VMEM = pl.BlockSpec(memory_space=pltpu.VMEM)
DMA = pltpu.SemaphoreType.DMA


def head_scratch():
    return [pltpu.VMEM((2 * ROWS, HALF), F32)] * 4 + [pltpu.VMEM((ROWS, HEAD), F32)] * 2


def local_call(pos, x, gains, freq, wq, wk, wv, wo, kc, vc):
    groups, n = ROWS // GROUP, kc.shape[1]
    table = pltpu.VMEM((ROWS, HALF), F32)
    return pl.pallas_call(
        local_kernel,
        name="local_attention",
        out_shape=(jax.ShapeDtypeStruct(kc.shape, BF16), jax.ShapeDtypeStruct(vc.shape, BF16),
                   pltpu.VMEM((2, ROWS, SIDE), BF16), table, table, pltpu.VMEM(x.shape, BF16)),
        in_specs=[ANY] * 10,
        out_specs=(IN_HBM, IN_HBM, IN_VMEM, IN_VMEM, IN_VMEM, IN_VMEM),
        scratch_shapes=[
            pltpu.SMEM((ROWS,), jnp.int32),
            pltpu.VMEM((4, D), F32), pltpu.VMEM((1, HALF), F32),
            pltpu.VMEM((D, 2 * HEAD), BF16), pltpu.VMEM((D, HEAD), BF16), pltpu.VMEM((D, HEAD), BF16), pltpu.VMEM((2 * HEAD, D), BF16),
            pltpu.VMEM((groups, GROUP, n, HEAD), BF16), pltpu.VMEM((groups, GROUP, n, HEAD), BF16),
        ] + head_scratch() + [DMA((4,)), DMA((4,))] + [DMA((groups,))] * 4,
        compiler_params=pltpu.CompilerParams(vmem_limit_bytes=40 * MIB),
    )(*[in_hbm(v) for v in (pos, x, gains, freq, wq, wk, wv, wo, kc, vc)])


def global_call(pos, a, cos_part, sin_part, ahead, kc, vc):
    groups, n = ROWS // GROUP, kc.shape[1]
    first = (pltpu.VMEM((GROUP, n, HEAD), BF16),) * (2 * FIRST)
    rest = groups - FIRST
    return pl.pallas_call(
        global_kernel,
        name="global_attention",
        out_shape=(jax.ShapeDtypeStruct(kc.shape, BF16), jax.ShapeDtypeStruct(vc.shape, BF16),
                   pltpu.VMEM((2, ROWS, SIDE), BF16)) + first,
        in_specs=[ANY] + [IN_VMEM] * (7 + 2 * FIRST) + [ANY] * 2,
        out_specs=(IN_HBM, IN_HBM) + (IN_VMEM,) * (1 + 2 * FIRST),
        input_output_aliases={8 + i: 3 + i for i in range(2 * FIRST)},
        scratch_shapes=[
            pltpu.SMEM((ROWS,), jnp.int32),
            pltpu.VMEM((rest, GROUP, n, HEAD), BF16), pltpu.VMEM((rest, GROUP, n, HEAD), BF16),
        ] + head_scratch() + [DMA(())] + [DMA((rest,))] * 2 + [DMA((groups,))] * 2,
        compiler_params=pltpu.CompilerParams(vmem_limit_bytes=27 * MIB),
    )(in_hbm(pos), *[in_vmem(v) for v in (a, cos_part, sin_part, *ahead)], in_hbm(kc), in_hbm(vc))


def mlp_call(layer, x, o, gains, wg, wu, wd, ahead=()):
    full = pltpu.VMEM((ROWS, D), BF16)
    side = pltpu.VMEM((ROWS, SIDE), BF16)
    both = pltpu.VMEM((2, ROWS, SIDE), BF16)
    rows = pltpu.VMEM((ROWS, D), BF16)
    out_shape = [rows]
    if ahead:
        out_shape += [rows] + [pltpu.VMEM(w.shape[1:], BF16) for w in ahead[:4]]
        out_shape += [pltpu.VMEM((GROUP,) + c.shape[1:], BF16) for c in ahead[4:] for _ in range(FIRST)]
    return pl.pallas_call(
        functools.partial(mlp_kernel, layer),
        name=f"mlp{layer}",
        out_shape=out_shape,
        in_specs=[IN_VMEM] * 2 + [ANY] * (4 + len(ahead)),
        out_specs=[IN_VMEM] * len(out_shape),
        scratch_shapes=[
            full, pltpu.VMEM((2, 4, D), F32), pltpu.VMEM((D, FF_PART), BF16), pltpu.VMEM((D, FF_PART), BF16), pltpu.VMEM((FF_PART, D), BF16),
            pltpu.VMEM((2 * ROWS, D), BF16), pltpu.VMEM((2 * ROWS, FF_PART), BF16),
            full, side, side, side, side, side, pltpu.VMEM((2, 2, ROWS, SIDE), BF16),
            pltpu.VMEM((2, 2, ROWS, SIDE), BF16), both, both, side, side, side, both,
            DMA(()), DMA((3,)), DMA((4 + 2 * FIRST,)), DMA((5,)), DMA((5,)), DMA((2,)), DMA((2,)), DMA((5,)), DMA((5,)),
        ],
        compiler_params=pltpu.CompilerParams(collective_id=layer, has_side_effects=True, vmem_limit_bytes=24 * MIB),
    )(in_vmem(x), in_vmem(o), *[in_hbm(v) for v in (gains, wg, wu, wd) + tuple(ahead)])


def decode_step(hidden, positions, k_local, v_local, k_global, v_global, w_query, w_key, w_value, w_out, w_gate, w_up, w_down, norm_scale):
    freq = jnp.asarray((ROPE_BASE ** (-2.0 * np.arange(HALF) / HEAD)).astype(np.float32).reshape(1, HALF))

    def flat(cache):
        return cache.reshape(cache.shape[0], cache.shape[1], HEAD)

    kg, vg = flat(k_global), flat(v_global)
    kl_new, vl_new, o, cos_part, sin_part, x = local_call(positions, hidden, norm_scale, freq, w_query, w_key, w_value, w_out, flat(k_local), flat(v_local))
    x, a, *ahead = mlp_call(0, x, o, norm_scale, w_gate, w_up, w_down, (w_query, w_key, w_value, w_out, kg, vg))
    kg_new, vg_new, o, *_ = global_call(positions, a, cos_part, sin_part, ahead, kg, vg)
    (x,) = mlp_call(1, x, o, norm_scale, w_gate, w_up, w_down)
    return (x, kl_new.reshape(k_local.shape), vl_new.reshape(v_local.shape), kg_new.reshape(k_global.shape), vg_new.reshape(v_global.shape))


def solution(mesh):
    row_spec = P('dp', None)
    cache_spec = P('dp', None, 'tp', None)
    col_split = P(None, None, 'tp')
    row_split = P(None, 'tp', None)
    in_specs = (row_spec, P('dp'), cache_spec, cache_spec, cache_spec, cache_spec, col_split, col_split, col_split, row_split, col_split, col_split, row_split, P())
    out_specs = (row_spec, cache_spec, cache_spec, cache_spec, cache_spec)
    return jax.shard_map(decode_step, mesh=mesh, in_specs=in_specs, out_specs=out_specs, check_vma=False)
```

```python
import functools

import jax
import jax.numpy as jnp
import numpy as np
from jax import lax
from jax.experimental import pallas as pl
from jax.experimental.pallas import tpu as pltpu
from jax.sharding import PartitionSpec as P

SOFT_CAP = 50.0
NORM_EPS = 1e-6
ROPE_BASE = 10000.0
ROWS = 24
D = 2560
HEAD = 256
HALF = 128
GROUP = 4
CHUNK = 512
SIDE = D // 2
MIB = 2 ** 20
FIRST = 3
FF_PART = D // 2
PIECE = 256
PARTS = ((0, 512), (512, 768))
F32 = jnp.float32
BF16 = jnp.bfloat16


def normed(values, gain_row):
    inv_rms = lax.rsqrt(jnp.mean(values * values, axis=-1, keepdims=True) + NORM_EPS)
    return (values * inv_rms * (1.0 + gain_row)).astype(BF16)


def rotation(pos, freq):
    row_ids = lax.broadcasted_iota(jnp.int32, (ROWS, HALF), 0)
    pos_rows = jnp.zeros((ROWS, HALF), jnp.int32)
    for b in range(ROWS):
        pos_rows = jnp.where(row_ids == b, pos[b], pos_rows)
    angles = pos_rows.astype(F32) * freq
    return jnp.cos(angles), jnp.sin(angles)


def rotate(t, cos_part, sin_part):
    first, second = t[:, :HALF], t[:, HALF:]
    return first * cos_part - second * sin_part, second * cos_part + first * sin_part


def store_queries(q, cos_part, sin_part, qa, qb):
    for h in range(2):
        first, second = rotate(q[:, h * HEAD:(h + 1) * HEAD], cos_part, sin_part)
        qa[pl.ds(h, ROWS, stride=2), :] = first
        qb[pl.ds(h, ROWS, stride=2), :] = second


def store_key(k, cos_part, sin_part, knew):
    first, second = rotate(k, cos_part, sin_part)
    knew[:, :HALF] = first
    knew[:, HALF:] = second


def patch(buf, j, row, b, new):
    base = pl.multiple_of((row // 16) * 16, 16)
    tile = buf[j, pl.ds(base, 16), :].astype(F32)
    hit = lax.broadcasted_iota(jnp.int32, (16, HEAD), 0) == row - base
    fresh = jnp.broadcast_to(new[pl.ds(b, 1), :], (16, HEAD))
    buf[j, pl.ds(base, 16), :] = jnp.where(hit, fresh, tile).astype(BF16)


def attend_group(masked, g, pos, kref, vref, wait_k, wait_v, qa, qb, ma, mb, knew, vnew):
    n = kref.shape[1]
    rows8 = pl.ds(g * 8 if isinstance(g, int) else pl.multiple_of(g * 8, 8), 8)
    wait_k()
    for j in range(GROUP):
        b = g * GROUP + j
        patch(kref, j, lax.rem(pos[b], n), b, knew)
    q8 = jnp.concatenate([qa[rows8, :], qb[rows8, :]], axis=1).astype(BF16)
    owner = lax.broadcasted_iota(jnp.int32, (8, n), 0) // 2
    s = None
    for j in range(GROUP):
        part = lax.dot_general(q8, kref[j], (((1,), (1,)), ((), ())), preferred_element_type=F32)
        s = part if s is None else jnp.where(owner == j, part, s)
    e = jnp.exp(SOFT_CAP * jnp.tanh(s * (HEAD ** -0.5 / SOFT_CAP)))
    if masked:
        limit_rows = lax.broadcasted_iota(jnp.int32, (8, 1), 0) // 2
        limit = jnp.zeros((8, 1), jnp.int32)
        for j in range(GROUP):
            limit = jnp.where(limit_rows == j, pos[g * GROUP + j], limit)
        e = jnp.where(lax.broadcasted_iota(jnp.int32, (8, n), 1) <= limit, e, 0.0)
    p = (e / jnp.sum(e, axis=-1, keepdims=True)).astype(BF16)
    wait_v()
    for j in range(GROUP):
        b = g * GROUP + j
        patch(vref, j, lax.rem(pos[b], n), b, vnew)
    owner = lax.broadcasted_iota(jnp.int32, (8, HEAD), 0) // 2
    m = None
    for j in range(GROUP):
        part = jnp.dot(p, vref[j], preferred_element_type=F32)
        m = part if m is None else jnp.where(owner == j, part, m)
    ma[rows8, :] = m[:, :HALF]
    mb[rows8, :] = m[:, HALF:]


def project_out(ma, mb, wo, o_ref):
    mixed = jnp.concatenate([ref[pl.ds(h, ROWS, stride=2), :] for h in range(2) for ref in (ma, mb)], axis=1).astype(BF16)
    for c in range(2):
        o_ref[c] = jnp.dot(mixed, wo[:, c * SIDE:(c + 1) * SIDE], preferred_element_type=F32).astype(BF16)


def group_rows(ref, g):
    return ref.at[pl.ds(g * GROUP, GROUP)]


def local_kernel(pos_hbm, x_hbm, gain_hbm, freq_hbm, wq_hbm, wk_hbm, wv_hbm, wo_hbm, kc_hbm, vc_hbm,
                 ko_hbm, vo_hbm, o_ref, cos_ref, sin_ref, x,
                 pos, gain, freq, wq, wk, wv, wo, kbuf, vbuf, qa, qb, ma, mb, knew, vnew,
                 small_sem, w_sem, kr_sem, vr_sem, kw_sem, vw_sem):
    groups = ROWS // GROUP
    small = [pltpu.make_async_copy(s, d, small_sem.at[i]) for i, (s, d) in enumerate(
        ((x_hbm, x), (gain_hbm.at[0], gain), (pos_hbm, pos), (freq_hbm, freq)))]
    weights = [pltpu.make_async_copy(s.at[0], d, w_sem.at[i]) for i, (s, d) in enumerate(
        ((wq_hbm, wq), (wk_hbm, wk), (wv_hbm, wv), (wo_hbm, wo)))]

    def k_read(g):
        return pltpu.make_async_copy(group_rows(kc_hbm, g), kbuf.at[g], kr_sem.at[g])

    def v_read(g):
        return pltpu.make_async_copy(group_rows(vc_hbm, g), vbuf.at[g], vr_sem.at[g])

    def writes(g):
        return (pltpu.make_async_copy(kbuf.at[g], group_rows(ko_hbm, g), kw_sem.at[g]),
                pltpu.make_async_copy(vbuf.at[g], group_rows(vo_hbm, g), vw_sem.at[g]))

    for copy in small:
        copy.start()
    for copy in weights[:3]:
        copy.start(priority=1)
    for g in range(groups):
        k_read(g).start(priority=1)
        v_read(g).start(priority=1)
    weights[3].start(priority=1)

    for copy in small:
        copy.wait()
    cos_part, sin_part = rotation(pos, freq[...])
    cos_ref[...] = cos_part
    sin_ref[...] = sin_part
    a = normed(x[...].astype(F32), gain[0:1, :])
    weights[0].wait()
    store_queries(jnp.dot(a, wq[...], preferred_element_type=F32), cos_part, sin_part, qa, qb)
    weights[1].wait()
    store_key(jnp.dot(a, wk[...], preferred_element_type=F32), cos_part, sin_part, knew)
    weights[2].wait()
    vnew[...] = jnp.dot(a, wv[...], preferred_element_type=F32)

    def step(g, carry):
        attend_group(False, g, pos, kbuf.at[g], vbuf.at[g], lambda: k_read(g).wait(), lambda: v_read(g).wait(), qa, qb, ma, mb, knew, vnew)
        for copy in writes(g):
            copy.start(priority=1)
        return carry

    lax.fori_loop(0, groups, step, 0)
    weights[3].wait()
    project_out(ma, mb, wo, o_ref)
    for g in range(groups):
        for copy in writes(g):
            copy.wait()


def global_kernel(pos_hbm, a_ref, cos_ref, sin_ref, wq, wk, wv, wo, *refs):
    kc_hbm, vc_hbm, ko_hbm, vo_hbm, o_ref = refs[2 * FIRST:2 * FIRST + 5]
    kfirst, vfirst = refs[2 * FIRST + 5:3 * FIRST + 5], refs[3 * FIRST + 5:4 * FIRST + 5]
    pos, kbuf, vbuf, qa, qb, ma, mb, knew, vnew, pos_sem, kr_sem, vr_sem, kw_sem, vw_sem = refs[4 * FIRST + 5:]
    groups = ROWS // GROUP
    pos_copy = pltpu.make_async_copy(pos_hbm, pos, pos_sem)

    def k_read(g):
        return pltpu.make_async_copy(group_rows(kc_hbm, g), kbuf.at[g - FIRST], kr_sem.at[g - FIRST])

    def v_read(g):
        return pltpu.make_async_copy(group_rows(vc_hbm, g), vbuf.at[g - FIRST], vr_sem.at[g - FIRST])

    def writes(g, k, v):
        return (pltpu.make_async_copy(k, group_rows(ko_hbm, g), kw_sem.at[g]),
                pltpu.make_async_copy(v, group_rows(vo_hbm, g), vw_sem.at[g]))

    pos_copy.start()
    for g in range(FIRST, groups):
        k_read(g).start(priority=1)
        v_read(g).start(priority=1)
    cos_part, sin_part = cos_ref[...], sin_ref[...]
    a = a_ref[...]
    store_queries(jnp.dot(a, wq[...], preferred_element_type=F32), cos_part, sin_part, qa, qb)
    store_key(jnp.dot(a, wk[...], preferred_element_type=F32), cos_part, sin_part, knew)
    vnew[...] = jnp.dot(a, wv[...], preferred_element_type=F32)
    pos_copy.wait()

    for g in range(FIRST):
        attend_group(True, g, pos, kfirst[g], vfirst[g], lambda: None, lambda: None, qa, qb, ma, mb, knew, vnew)
    for g in range(FIRST):
        for copy in writes(g, kfirst[g], vfirst[g]):
            copy.start(priority=1)

    def step(g, carry):
        k, v = kbuf.at[g - FIRST], vbuf.at[g - FIRST]
        attend_group(True, g, pos, k, v, lambda: k_read(g).wait(), lambda: v_read(g).wait(), qa, qb, ma, mb, knew, vnew)
        for copy in writes(g, k, v):
            copy.start(priority=1)
        return carry

    lax.fori_loop(FIRST, groups, step, 0)
    project_out(ma, mb, wo, o_ref)
    for g in range(groups):
        k, v = (kfirst[g], vfirst[g]) if g < FIRST else (kbuf.at[g - FIRST], vbuf.at[g - FIRST])
        for copy in writes(g, k, v):
            copy.wait()


def mlp_kernel(layer, *refs):
    n_in, n_out = (12, 6 + 2 * FIRST) if layer == 0 else (6, 1)
    x_ref, o_ref, gain_hbm, wg_hbm, wu_hbm, wd_hbm = refs[:6]
    outs = refs[n_in:n_in + n_out]
    (x, gain, wg, wu, wd, a48, h, x_other, opart, ohalf, ox, oy, oz, osum, fpart, fpair, fhalf, fx, fy, fz, fsum,
     small_sem, w_sem, ahead_sem, o_send, o_recv, x_send, x_recv, f_send, f_recv) = refs[n_in + n_out:]
    out_ref = outs[0]
    dp, me = lax.axis_index("dp"), lax.axis_index("tp")
    chip, core = me // 2, lax.rem(me, 2)
    side = lax.rem(chip + core, 2)
    partner = {"dp": dp, "tp": chip * 2 + (1 - core)}
    along = {"dp": dp, "tp": (1 - chip) * 2 + (1 - core)}
    beside = {"dp": 1 - dp, "tp": chip * 2 + core}
    opposite = {"dp": 1 - dp, "tp": (1 - chip) * 2 + (1 - core)}

    part = pl.ds(pl.multiple_of(dp * FF_PART, FF_PART), FF_PART)
    weights = [pltpu.make_async_copy(s, d, w_sem.at[i]) for i, (s, d) in enumerate(
        ((wg_hbm.at[layer, :, part], wg), (wu_hbm.at[layer, :, part], wu), (wd_hbm.at[layer, part, :], wd)))]
    gain_copy = pltpu.make_async_copy(gain_hbm, gain, small_sem)
    ahead = []
    if layer == 0:
        wq_hbm, wk_hbm, wv_hbm, wo_hbm, kc_hbm, vc_hbm = refs[6:12]
        pairs = list(zip([w.at[1] for w in (wq_hbm, wk_hbm, wv_hbm, wo_hbm)], outs[2:6]))
        for g in range(FIRST):
            pairs += [(group_rows(kc_hbm, g), outs[6 + g]), (group_rows(vc_hbm, g), outs[6 + FIRST + g])]
        ahead = [pltpu.make_async_copy(s, d, ahead_sem.at[i]) for i, (s, d) in enumerate(pairs)]

    gain_copy.start()
    for copy in weights:
        copy.start(priority=1)

    barrier = pltpu.get_barrier_semaphore()
    for peer in (partner, along, beside, opposite):
        pl.semaphore_signal(barrier, inc=1, device_id=peer, device_id_type=pl.DeviceIdType.MESH)
    pl.semaphore_wait(barrier, 4)

    def remote(src, dst, send, recv, peer):
        return pltpu.make_async_remote_copy(src_ref=src, dst_ref=dst, send_sem=send, recv_sem=recv,
                                            device_id=peer, device_id_type=pl.DeviceIdType.MESH)

    mine = pl.ds(pl.multiple_of(side * SIDE, SIDE), SIDE)
    theirs = pl.ds(pl.multiple_of((1 - side) * SIDE, SIDE), SIDE)

    o_copies = [remote(src, dst, o_send.at[i], o_recv.at[i], peer) for i, (src, dst, peer) in enumerate((
        (o_ref.at[1 - side], opart, partner), (ohalf, oz, opposite), (ohalf, oy, beside), (ohalf, ox, along),
        (osum.at[side], osum.at[side], partner)))]
    x_copies = [remote(src, dst, x_send.at[i], x_recv.at[i], peer) for i, (src, dst, peer) in enumerate((
        (x_ref.at[:, mine], x_other.at[:, mine], beside), (x_other.at[:, mine], x_other.at[:, mine], partner)))]
    o_copies[0].start()
    x_copies[0].start()
    for copy in ahead:
        copy.start(priority=1)
    gain_copy.wait()
    o_copies[0].wait_recv()
    ohalf[...] = (o_ref[side].astype(F32) + opart[...].astype(F32)).astype(BF16)
    for copy in o_copies[1:4]:
        copy.start()
    x_copies[0].wait_recv()
    x_copies[1].start()
    for copy in o_copies[1:4]:
        copy.wait_recv()
    osum[side, 0] = (ohalf[...].astype(F32) + ox[...].astype(F32)).astype(BF16)
    osum[side, 1] = (oy[...].astype(F32) + oz[...].astype(F32)).astype(BF16)
    o_copies[4].start()
    x_copies[1].wait_recv()
    o_copies[4].wait_recv()
    for group, rows in enumerate((x_ref, x_other)):
        o_rows = jnp.concatenate([osum[0, group], osum[1, group]], axis=1).astype(F32)
        x1 = (rows[...].astype(F32) + normed(o_rows, gain[layer, 1:2, :]).astype(F32)).astype(BF16)
        if group == 0:
            x[...] = x1
        a48[group * ROWS:(group + 1) * ROWS, :] = normed(x1.astype(F32), gain[layer, 2:3, :])
    weights[0].wait()
    weights[1].wait()
    a = a48[...]
    for c in range(0, FF_PART, PIECE):
        gate = jnp.dot(a, wg[:, c:c + PIECE], preferred_element_type=F32)
        up = jnp.dot(a, wu[:, c:c + PIECE], preferred_element_type=F32)
        h[:, c:c + PIECE] = (jax.nn.gelu(gate, approximate=True) * up).astype(BF16)
    weights[2].wait()
    act = h[...]

    def f_exchange(j):
        cut = pl.ds(*PARTS[j])
        return [remote(src, dst, f_send.at[j, i], f_recv.at[j, i], peer) for i, (src, dst, peer) in enumerate((
            (fpart.at[1 - side, :, :, cut], fpair.at[:, :, cut], partner), (fhalf.at[1, :, cut], fz.at[:, cut], opposite),
            (fhalf.at[1, :, cut], fy.at[:, cut], beside), (fhalf.at[0, :, cut], fx.at[:, cut], along),
            (fsum.at[side, :, cut], fsum.at[side, :, cut], partner)))]

    f_copies = [f_exchange(j) for j in range(len(PARTS))]

    def down(which, j):
        start, size = PARTS[j]
        columns = pl.ds(pl.multiple_of(which * SIDE + start, PIECE), size)
        partial = jnp.dot(act, wd[:, columns], preferred_element_type=F32)
        for group in range(2):
            fpart[which, group, :, start:start + size] = partial[group * ROWS:(group + 1) * ROWS].astype(BF16)

    for j, copies in enumerate(f_copies):
        down(1 - side, j)
        copies[0].start()
    for j, copies in enumerate(f_copies):
        cut = pl.ds(*PARTS[j])
        down(side, j)
        copies[0].wait_recv()
        for group in (1, 0):
            fhalf[group, :, cut] = (fpart[side, group, :, cut].astype(F32) + fpair[group, :, cut].astype(F32)).astype(BF16)
        for copy in copies[1:4]:
            copy.start()
    for j, copies in enumerate(f_copies):
        cut = pl.ds(*PARTS[j])
        for copy in copies[1:4]:
            copy.wait_recv()
        near = fhalf[0, :, cut].astype(F32) + fx[:, cut].astype(F32)
        fsum[side, :, cut] = (near + (fy[:, cut].astype(F32) + fz[:, cut].astype(F32))).astype(BF16)
        copies[4].start()
    for copies in f_copies:
        copies[4].wait_recv()
    f_rows = jnp.concatenate([fsum[0], fsum[1]], axis=1).astype(F32)
    x2 = (x[...].astype(F32) + normed(f_rows, gain[layer, 3:4, :]).astype(F32)).astype(BF16)
    out_ref[...] = x2
    if layer == 0:
        outs[1][...] = normed(x2.astype(F32), gain[1, 0:1, :])
    for copy in o_copies + x_copies + f_copies[0] + f_copies[1]:
        copy.wait_send()
    for copy in ahead:
        copy.wait()


def in_hbm(value):
    return pltpu.with_memory_space_constraint(value, pltpu.HBM)


def in_vmem(value):
    return pltpu.with_memory_space_constraint(value, pltpu.VMEM)


ANY = pl.BlockSpec(memory_space=pl.ANY)
IN_HBM = pl.BlockSpec(memory_space=pltpu.HBM)
IN_VMEM = pl.BlockSpec(memory_space=pltpu.VMEM)
DMA = pltpu.SemaphoreType.DMA


def head_scratch():
    return [pltpu.VMEM((2 * ROWS, HALF), F32)] * 4 + [pltpu.VMEM((ROWS, HEAD), F32)] * 2


def local_call(pos, x, gains, freq, wq, wk, wv, wo, kc, vc):
    groups, n = ROWS // GROUP, kc.shape[1]
    table = pltpu.VMEM((ROWS, HALF), F32)
    return pl.pallas_call(
        local_kernel,
        name="local_attention",
        out_shape=(jax.ShapeDtypeStruct(kc.shape, BF16), jax.ShapeDtypeStruct(vc.shape, BF16),
                   pltpu.VMEM((2, ROWS, SIDE), BF16), table, table, pltpu.VMEM(x.shape, BF16)),
        in_specs=[ANY] * 10,
        out_specs=(IN_HBM, IN_HBM, IN_VMEM, IN_VMEM, IN_VMEM, IN_VMEM),
        scratch_shapes=[
            pltpu.SMEM((ROWS,), jnp.int32),
            pltpu.VMEM((4, D), F32), pltpu.VMEM((1, HALF), F32),
            pltpu.VMEM((D, 2 * HEAD), BF16), pltpu.VMEM((D, HEAD), BF16), pltpu.VMEM((D, HEAD), BF16), pltpu.VMEM((2 * HEAD, D), BF16),
            pltpu.VMEM((groups, GROUP, n, HEAD), BF16), pltpu.VMEM((groups, GROUP, n, HEAD), BF16),
        ] + head_scratch() + [DMA((4,)), DMA((4,))] + [DMA((groups,))] * 4,
        compiler_params=pltpu.CompilerParams(vmem_limit_bytes=40 * MIB),
    )(*[in_hbm(v) for v in (pos, x, gains, freq, wq, wk, wv, wo, kc, vc)])


def global_call(pos, a, cos_part, sin_part, ahead, kc, vc):
    groups, n = ROWS // GROUP, kc.shape[1]
    first = (pltpu.VMEM((GROUP, n, HEAD), BF16),) * (2 * FIRST)
    rest = groups - FIRST
    return pl.pallas_call(
        global_kernel,
        name="global_attention",
        out_shape=(jax.ShapeDtypeStruct(kc.shape, BF16), jax.ShapeDtypeStruct(vc.shape, BF16),
                   pltpu.VMEM((2, ROWS, SIDE), BF16)) + first,
        in_specs=[ANY] + [IN_VMEM] * (7 + 2 * FIRST) + [ANY] * 2,
        out_specs=(IN_HBM, IN_HBM) + (IN_VMEM,) * (1 + 2 * FIRST),
        input_output_aliases={8 + i: 3 + i for i in range(2 * FIRST)},
        scratch_shapes=[
            pltpu.SMEM((ROWS,), jnp.int32),
            pltpu.VMEM((rest, GROUP, n, HEAD), BF16), pltpu.VMEM((rest, GROUP, n, HEAD), BF16),
        ] + head_scratch() + [DMA(())] + [DMA((rest,))] * 2 + [DMA((groups,))] * 2,
        compiler_params=pltpu.CompilerParams(vmem_limit_bytes=27 * MIB),
    )(in_hbm(pos), *[in_vmem(v) for v in (a, cos_part, sin_part, *ahead)], in_hbm(kc), in_hbm(vc))


def mlp_call(layer, x, o, gains, wg, wu, wd, ahead=()):
    full = pltpu.VMEM((ROWS, D), BF16)
    side = pltpu.VMEM((ROWS, SIDE), BF16)
    both = pltpu.VMEM((2, ROWS, SIDE), BF16)
    rows = pltpu.VMEM((ROWS, D), BF16)
    out_shape = [rows]
    if ahead:
        out_shape += [rows] + [pltpu.VMEM(w.shape[1:], BF16) for w in ahead[:4]]
        out_shape += [pltpu.VMEM((GROUP,) + c.shape[1:], BF16) for c in ahead[4:] for _ in range(FIRST)]
    return pl.pallas_call(
        functools.partial(mlp_kernel, layer),
        name=f"mlp{layer}",
        out_shape=out_shape,
        in_specs=[IN_VMEM] * 2 + [ANY] * (4 + len(ahead)),
        out_specs=[IN_VMEM] * len(out_shape),
        scratch_shapes=[
            full, pltpu.VMEM((2, 4, D), F32), pltpu.VMEM((D, FF_PART), BF16), pltpu.VMEM((D, FF_PART), BF16), pltpu.VMEM((FF_PART, D), BF16),
            pltpu.VMEM((2 * ROWS, D), BF16), pltpu.VMEM((2 * ROWS, FF_PART), BF16),
            full, side, side, side, side, side, pltpu.VMEM((2, 2, ROWS, SIDE), BF16),
            pltpu.VMEM((2, 2, ROWS, SIDE), BF16), both, both, side, side, side, both,
            DMA(()), DMA((3,)), DMA((4 + 2 * FIRST,)), DMA((5,)), DMA((5,)), DMA((2,)), DMA((2,)), DMA((2, 5)), DMA((2, 5)),
        ],
        compiler_params=pltpu.CompilerParams(collective_id=layer, has_side_effects=True, vmem_limit_bytes=24 * MIB),
    )(in_vmem(x), in_vmem(o), *[in_hbm(v) for v in (gains, wg, wu, wd) + tuple(ahead)])


def decode_step(hidden, positions, k_local, v_local, k_global, v_global, w_query, w_key, w_value, w_out, w_gate, w_up, w_down, norm_scale):
    freq = jnp.asarray((ROPE_BASE ** (-2.0 * np.arange(HALF) / HEAD)).astype(np.float32).reshape(1, HALF))

    def flat(cache):
        return cache.reshape(cache.shape[0], cache.shape[1], HEAD)

    kg, vg = flat(k_global), flat(v_global)
    kl_new, vl_new, o, cos_part, sin_part, x = local_call(positions, hidden, norm_scale, freq, w_query, w_key, w_value, w_out, flat(k_local), flat(v_local))
    x, a, *ahead = mlp_call(0, x, o, norm_scale, w_gate, w_up, w_down, (w_query, w_key, w_value, w_out, kg, vg))
    kg_new, vg_new, o, *_ = global_call(positions, a, cos_part, sin_part, ahead, kg, vg)
    (x,) = mlp_call(1, x, o, norm_scale, w_gate, w_up, w_down)
    return (x, kl_new.reshape(k_local.shape), vl_new.reshape(v_local.shape), kg_new.reshape(k_global.shape), vg_new.reshape(v_global.shape))


def solution(mesh):
    row_spec = P('dp', None)
    cache_spec = P('dp', None, 'tp', None)
    col_split = P(None, None, 'tp')
    row_split = P(None, 'tp', None)
    in_specs = (row_spec, P('dp'), cache_spec, cache_spec, cache_spec, cache_spec, col_split, col_split, col_split, row_split, col_split, col_split, row_split, P())
    out_specs = (row_spec, cache_spec, cache_spec, cache_spec, cache_spec)
    return jax.shard_map(decode_step, mesh=mesh, in_specs=in_specs, out_specs=out_specs, check_vma=False)
```
